32 devices in a mesh: slab: 8 (over z, x), cross: 4 (over y, core).
Axes of the slice: x: 2, y: 2, z: 4, core: 2. Of those that a mesh axis runs over, the one named last changes fastest.
Arguments:
- gas_state: float32 [16, 64, 8192], P(None, 'slab', 'cross'), may hold values from -4 to 4, as said below
- parcel_record: float32 [5, 131072], P(None, ('slab', 'cross')), may hold values from -4 to 4, as said below
- condensed_shares: float32 [12, 131072], P(None, ('slab', 'cross')), may hold values from 0.02 to 0.2
- surface_steam_factor: float32 [12], replicated, may hold values from 0.2 to 2
- fine_cell: int32 [131072], P(('slab', 'cross')), may hold values from 0 to 20479, as said below
- block_counts: int32 [1024], P(('slab', 'cross')), may hold values from 16 to 128, as said below
Outputs:
- parcel_next: float32 [5, 131072], P(None, ('slab', 'cross'))
- fine_source: float32 [16, 64, 8192], P(None, 'slab', 'cross')
- correction: float32 [64, 4096], replicated
The draws below stay inside these ranges and needn't reach their ends.
Inputs may be any that keep to these rules, and one draw needn't show every extreme that they name: fine_cell is plane * 2048 + k, with plane 0 and 9 the neighbouring slabs' last and first planes; it never points outside the gas mesh, and is non-decreasing over each device's 4096 slots. The live parcels of each aligned block of 128 slots are its first block_counts slots; the last block of each device's 4096 slots is full. `gas_state`: rows 0 to 2 velocity, row 3 temperature from 1 to 2, rows 4 on vapour fractions from 0 to 0.1. `parcel_record`: rows 0 to 2 velocity, row 3 temperature from 0.6 to 0.9, row 4 mass from 0.5 to 3.
All inputs are finite; a program needn't handle non-finite values.
Results may differ from the reference program's by a relative error of at most 0.00002.
Values sent between devices are 32-bit elements; how exact they have to be, the bound alone decides.
No kernel may reach another device: no remote copies, remote signals or barrier semaphores. Data moves between devices by JAX's collectives and lax.ppermute only.
A program may use at most 64 MiB of HBM per device.

```python
import math
import jax
import jax.numpy as jnp

SPECIES = 12
PLANES = 8
CROSS_CELLS = 2048
PAR_DEV = 4096
BLOCK = 128
COARSE = 64
SWEEPS = 4
PTOT = 131072
N_SLAB = 8
N_CROSS = 4


def draw_gas_state(key, part):
    domain_layer_sequence = PLANES * N_SLAB
    traversed_mesh_sites_whole = CROSS_CELLS * N_CROSS
    key_velocity = jax.random.fold_in(key, 11)
    thermal_noise_seed = jax.random.fold_in(key, 12)
    key_vapour = jax.random.fold_in(key, 13)
    motion_components = jnp.clip(jax.random.normal(key_velocity, (3, domain_layer_sequence, traversed_mesh_sites_whole), jnp.float32), -4.0, 4.0)
    thermal_reading = jax.random.uniform(thermal_noise_seed, (1, domain_layer_sequence, traversed_mesh_sites_whole), jnp.float32, 1.0, 2.0)
    steam_share = jax.random.uniform(key_vapour, (SPECIES, domain_layer_sequence, traversed_mesh_sites_whole), jnp.float32, 0.0, 0.1)
    return jnp.concatenate([motion_components, thermal_reading, steam_share], axis=0)


def draw_parcel_record(key, part):
    position_number_whole = PAR_DEV * N_SLAB * N_CROSS
    key_velocity = jax.random.fold_in(key, 21)
    thermal_noise_seed = jax.random.fold_in(key, 22)
    key_weight = jax.random.fold_in(key, 23)
    motion_components = jnp.clip(jax.random.normal(key_velocity, (3, position_number_whole), jnp.float32), -4.0, 4.0)
    thermal_reading = jax.random.uniform(thermal_noise_seed, (1, position_number_whole), jnp.float32, 0.6, 0.9)
    natural_log_weight = jax.random.uniform(key_weight, (1, position_number_whole), jnp.float32, jnp.log(0.5), jnp.log(3.0))
    return jnp.concatenate([motion_components, thermal_reading, jnp.exp(natural_log_weight)], axis=0)


def draw_fine_cell(key, part):
    devices_all = N_SLAB * N_CROSS
    slab_ids = jnp.arange(devices_all, dtype=jnp.int32) // N_CROSS
    lowest = jnp.where(slab_ids == 0, 1, 0).astype(jnp.int32)
    highest = jnp.where(slab_ids == N_SLAB - 1, PLANES, PLANES + 1).astype(jnp.int32)
    key_plane = jax.random.fold_in(key, 31)
    key_column = jax.random.fold_in(key, 32)
    plane_drawn = jax.random.randint(key_plane, (devices_all, PAR_DEV), lowest[:, None], highest[:, None] + 1, jnp.int32)
    column_drawn = jax.random.randint(key_column, (devices_all, PAR_DEV), 0, CROSS_CELLS, jnp.int32)
    cells = jnp.sort(plane_drawn * CROSS_CELLS + column_drawn, axis=1)
    return cells.reshape(-1).astype(jnp.int32)


def draw_block_counts(key, part):
    blocks_all = PAR_DEV * N_SLAB * N_CROSS // BLOCK
    blocks_device = PAR_DEV // BLOCK
    block_ids = jnp.arange(blocks_all, dtype=jnp.int32)
    slab_ids = block_ids // blocks_device // N_CROSS
    last_block = block_ids % blocks_device == blocks_device - 1
    dense_slabs = max(1, N_SLAB // 4)
    lowest = jnp.where((slab_ids < dense_slabs) | last_block, BLOCK, 16).astype(jnp.int32)
    return jax.random.randint(jax.random.fold_in(key, 41), (blocks_all,), lowest, BLOCK + 1, jnp.int32)


def block_levels(stream_key, shape, cuts, low, top_value):
    factor_of, own = 1.0, jax.random.fold_in(stream_key, 6)
    for axis_at, parts in cuts:
        heights = jnp.exp(jax.random.uniform(jax.random.fold_in(own, axis_at), (parts,), jnp.float32, low / len(cuts), top_value / len(cuts)))
        factor_of = factor_of * jnp.repeat(heights, shape[axis_at] // parts).reshape([-1 if axis == axis_at else 1 for axis in range(len(shape))])
    return factor_of


def setup_inputs(seed: int = 0) -> dict:
    splits = jax.random.split(jax.random.key(seed), 7)
    gas_state = draw_gas_state(jax.random.fold_in(splits[6], 71), 0)
    parcel_record = draw_parcel_record(jax.random.fold_in(splits[6], 71), 0)
    condensed_shares = jnp.clip(0.02 + 0.18 * jax.random.uniform(splits[2], (SPECIES, PTOT), jnp.float32) ** block_levels(splits[2], (SPECIES, PTOT), ((1, 32),), -0.2, 0.2), 0.02, 0.2)
    surface_steam_factor = jnp.clip(jnp.exp(jax.random.uniform(splits[3], (SPECIES,), jnp.float32, math.log(0.2), math.log(2.0))), 0.2, 2.0)
    fine_cell = draw_fine_cell(jax.random.fold_in(splits[6], 71), 0)
    block_counts = draw_block_counts(jax.random.fold_in(splits[6], 71), 0)
    return {"gas_state": gas_state, "parcel_record": parcel_record, "condensed_shares": condensed_shares, "surface_steam_factor": surface_steam_factor, "fine_cell": fine_cell, "block_counts": block_counts}


drag_rate = 0.5
evap_rate = 0.08
warming_speed = 0.3
latent_boiling_energy = 0.5
vapour_heat = 1.5
volume_inverse = 4.0


def advance(ambient_layer_fields, parcel_record, condensed_shares, surface_steam_factor, alive_mask):
    gas_velocity = ambient_layer_fields[0:3]
    ambient_thermal_level = ambient_layer_fields[3]
    gas_vapour = ambient_layer_fields[4:]
    parcel_velocity = parcel_record[0:3]
    parcel_thermal_level = parcel_record[3]
    parcel_weight_amount = parcel_record[4]
    slip_velocity = gas_velocity - parcel_velocity
    slip_squared = jnp.sum(slip_velocity * slip_velocity, axis=0)
    drag_factor = drag_rate * jnp.power(parcel_weight_amount, -2.0 / 3.0) * (1.0 + 0.15 * jnp.power(slip_squared + 1.0, 0.3435))
    following_motion = (parcel_velocity + drag_factor * gas_velocity) / (1.0 + drag_factor)
    surface_steam_share = condensed_shares * surface_steam_factor[:, None] * jnp.exp(2.0 * (parcel_thermal_level - 0.75))
    species_rates = evap_rate * parcel_weight_amount * (surface_steam_share - gas_vapour)
    evaporated_weight = jnp.sum(species_rates, axis=0)
    thermal_exchange = warming_speed * (ambient_thermal_level - parcel_thermal_level) * jnp.power(parcel_weight_amount, 1.0 / 3.0)
    following_thermal_level = parcel_thermal_level + (thermal_exchange - latent_boiling_energy * evaporated_weight) / parcel_weight_amount
    following_weight = parcel_weight_amount - evaporated_weight
    momentum_terms = parcel_weight_amount * (parcel_velocity - following_motion) + evaporated_weight * following_motion
    energy_terms = vapour_heat * evaporated_weight - thermal_exchange
    source_terms = jnp.concatenate([momentum_terms, energy_terms[None], species_rates], axis=0)
    source_terms = source_terms * (alive_mask * volume_inverse)
    updated_parcel_record = jnp.concatenate([following_motion, following_thermal_level[None], following_weight[None]], axis=0)
    parcel_next = jnp.where(alive_mask[None] > 0.5, updated_parcel_record, parcel_record)
    return source_terms, parcel_next, evaporated_weight * alive_mask


def neighbours(values_grid):
    edge = values_grid.shape[0]
    padded_x = jnp.pad(values_grid, ((1, 1), (0, 0)))
    summed = padded_x[2:] + padded_x[:-2]
    padded_y = jnp.pad(values_grid, ((0, 0), (edge, edge)))
    summed = summed + padded_y[:, 2 * edge:] + padded_y[:, :-2 * edge]
    padded_z = jnp.pad(values_grid, ((0, 0), (1, 1)))
    depth = jnp.arange(values_grid.shape[1], dtype=jnp.int32) % edge
    upper_mask = (depth < edge - 1).astype(values_grid.dtype)
    lower_mask = (depth > 0).astype(values_grid.dtype)
    return summed + padded_z[:, 2:] * upper_mask + padded_z[:, :-2] * lower_mask


def relax(coarse_source):
    solution = jnp.zeros_like(coarse_source)
    for sweep in range(SWEEPS):
        solution = (neighbours(solution) + coarse_source) / 6.0
    return solution


def reference(gas_state, parcel_record, condensed_shares, surface_steam_factor, fine_cell, block_counts):
    position_number_whole = parcel_record.shape[1]
    per_device = position_number_whole // (N_SLAB * N_CROSS)
    slot_ids = jnp.arange(position_number_whole, dtype=jnp.int32)
    device_ids = slot_ids // per_device
    slab_ids = device_ids // N_CROSS
    cross_ids = device_ids % N_CROSS
    alive_mask = ((slot_ids % BLOCK) < block_counts[slot_ids // BLOCK]).astype(jnp.float32)
    plane_ext = fine_cell // CROSS_CELLS
    column = fine_cell % CROSS_CELLS
    global_plane = slab_ids * PLANES + plane_ext - 1
    global_cross = cross_ids * CROSS_CELLS + column
    domain_layer_sequence = PLANES * N_SLAB
    traversed_mesh_sites_whole = CROSS_CELLS * N_CROSS
    global_index = (global_plane * traversed_mesh_sites_whole + global_cross).astype(jnp.int32)
    fields = gas_state.shape[0]
    gas_flat = gas_state.reshape(fields, domain_layer_sequence * traversed_mesh_sites_whole)
    ambient_layer_fields = jnp.take(gas_flat, global_index, axis=1)
    source_terms, parcel_next, evaporated_weight = advance(ambient_layer_fields, parcel_record, condensed_shares, surface_steam_factor, alive_mask)
    fine_source = jnp.zeros((fields, domain_layer_sequence * traversed_mesh_sites_whole), jnp.float32).at[:, global_index].add(source_terms)
    fine_source = fine_source.reshape(fields, domain_layer_sequence, traversed_mesh_sites_whole)
    squared = COARSE * COARSE
    fine_per_coarse = domain_layer_sequence // COARSE
    cross_per_coarse = traversed_mesh_sites_whole // squared
    coarse_index = ((global_plane // fine_per_coarse) * squared + global_cross // cross_per_coarse).astype(jnp.int32)
    coarse_source = jnp.zeros((COARSE * squared,), jnp.float32).at[coarse_index].add(evaporated_weight)
    coarse_source = coarse_source.reshape(COARSE, squared)
    correction = relax(coarse_source)
    return (parcel_next, fine_source, correction)
```

```python
import functools

import jax
import jax.numpy as jnp
from jax import lax
from jax.experimental import pallas as pl
from jax.experimental.pallas import tpu as pltpu
from jax.sharding import PartitionSpec as P

BLOCK = 128
COARSE = 64
SWEEPS = 4
LANES = 128
WIDE = 8
UNROLL = 4
AXES = ("slab", "cross")
F32 = jnp.float32
VMEM = pl.BlockSpec(memory_space=pltpu.VMEM)
SMEM = pl.BlockSpec(memory_space=pltpu.SMEM)

drag_rate = 0.5
evap_rate = 0.08
warming_speed = 0.3
latent_boiling_energy = 0.5
vapour_heat = 1.5
volume_inverse = 4.0


def rows_in(tile, species):
    return jnp.concatenate([tile[:, 4 : 4 + species], tile[:, 0:4]], axis=1)


def plane_sides():
    return lax.rem(lax.axis_index("slab"), 2) == 0


def edges_kernel(gas, first_pair, second_pair):
    fields, planes, cells = gas.shape
    even = plane_sides()
    for k in range(cells // LANES):
        x = jnp.swapaxes(gas[:, :, k * LANES : (k + 1) * LANES], 0, 1)
        low, high = (rows_in(x[p : p + 1], fields - 4)[0] for p in (0, planes - 1))
        first_pair[k] = jnp.where(even, high, low)
        second_pair[k] = jnp.where(even, low, high)


def tiles_kernel(gas, tiles):
    fields, planes, cells = gas.shape
    per_plane = cells // LANES
    for k in range(per_plane):
        x = jnp.swapaxes(gas[:, :, k * LANES : (k + 1) * LANES], 0, 1)
        x = rows_in(x, fields - 4)
        for p in range(planes):
            tiles[p * per_plane + k] = x[p]


def advance_block(g, record, shares, steam, count):
    species = shares.shape[0]
    lane = lax.broadcasted_iota(jnp.int32, (1, LANES), 1)
    row = lax.broadcasted_iota(jnp.int32, (8, LANES), 0)
    rest = species - 8
    zeros = jnp.zeros((8 - rest, LANES), F32)
    g0, g1 = g
    s0 = shares[0:8]
    s1 = jnp.concatenate([shares[8:species], zeros], axis=0)
    r = jnp.concatenate([zeros, record[0:4]], axis=0)
    thermal = record[3:4]
    mass = record[4:5]
    d = g1 - r
    moving = (row >= 4) & (row < 7)
    slip_squared = jnp.sum(jnp.where(moving, d * d, 0.0), axis=0, keepdims=True)
    log_mass = jnp.log(mass)
    drag = (
        drag_rate
        * jnp.exp(log_mass * (-2.0 / 3.0))
        * (1.0 + 0.15 * jnp.exp(0.3435 * jnp.log(slip_squared + 1.0)))
    )
    following = (r + drag * g1) / (1.0 + drag)
    vapour = jnp.exp(2.0 * (thermal - 0.75))
    scale = evap_rate * mass
    rate0 = scale * (s0 * steam[0:8] * vapour - g0)
    rate1 = scale * (s1 * steam[8:16] * vapour - g1)
    evap = jnp.sum(rate0 + jnp.where(row < rest, rate1, 0.0), axis=0, keepdims=True)
    heat = warming_speed * d[7:8] * jnp.exp(log_mass * (1.0 / 3.0))
    next_thermal = thermal + (heat - latent_boiling_energy * evap) / mass
    next_mass = mass - evap
    momentum = mass * (r - following) + evap * following
    energy = vapour_heat * evap - heat
    alive = lane < count
    weight = jnp.where(alive, volume_inverse, 0.0)
    terms0 = rate0 * weight
    terms1 = jnp.where(row < rest, rate1, jnp.where(row < 7, momentum, energy)) * weight
    updated = jnp.concatenate([following[4:7], next_thermal, next_mass], axis=0)
    return (terms0, terms1), jnp.where(alive, updated, record)


def three_parts(x):
    high = x.astype(jnp.bfloat16).astype(F32)
    x = x - high
    middle = x.astype(jnp.bfloat16).astype(F32)
    return high, middle, x - middle


def deposit(parts, tile_of, first, onehot, number, acc):
    stack = []
    for j in range(number):
        here = tile_of == first + j
        for t0, t1 in parts:
            both = jnp.concatenate([jnp.where(here, t0, 0.0), jnp.where(here, t1, 0.0)], axis=0)
            stack.append(both.astype(jnp.bfloat16))
    stack = jnp.concatenate(stack, axis=0)
    sums = lax.dot_general(
        stack, onehot, (((1,), (1,)), ((), ())), preferred_element_type=F32
    )
    rows = 16
    for j in range(number):
        base = j * len(parts) * rows
        total = sums[base : base + rows]
        for i in range(1, len(parts)):
            total = total + sums[base + i * rows : base + (i + 1) * rows]
        acc[first + j] = acc[first + j] + total


def parcels_kernel(
    cell_s, count_s, steam_s, cell_v, tiles, pair_a, pair_b, record, shares,
    next_record, acc, send_a, send_b, coarse, gas,
):
    per_plane = pair_a.shape[0]
    inner = tiles.shape[0]
    blocks = cell_v.shape[0]
    species = shares.shape[0]
    even = plane_sides()
    below = jnp.where(even, 1, 0)
    for k in range(per_plane):
        a, b = pair_a[k], pair_b[k]
        gas[k] = jnp.where(even, b, a)
        gas[per_plane + inner + k] = jnp.where(even, a, b)

    def fill(i, _):
        for u in range(8):
            gas[per_plane + i * 8 + u] = tiles[i * 8 + u]
        return 0

    lax.fori_loop(0, inner // 8, fill, 0)

    def clear(i, _):
        for u in range(8):
            acc[i * 8 + u] = jnp.zeros(acc.shape[1:], F32)
        return 0

    lax.fori_loop(0, acc.shape[0] // 8, clear, 0)

    species_row = lax.broadcasted_iota(jnp.int32, (16, 1), 0)
    steam = jnp.zeros((16, 1), F32)
    for j in range(species):
        steam = jnp.where(species_row == j, steam_s[j], steam)
    steam = jnp.broadcast_to(steam, (16, LANES))
    spot = lax.broadcasted_iota(jnp.int32, (LANES, LANES), 0)

    def prepare(b):
        cell = cell_v[pl.ds(b, 1), :]
        return cell // LANES, jnp.broadcast_to(lax.rem(cell, LANES), (8, LANES))

    def pick(tile, tile_of, offset, first, j, old):
        here = tile_of == first + j
        return tuple(
            jnp.where(here, jnp.take_along_axis(tile[h * 8 : h * 8 + 8], offset, axis=1), o)
            for h, o in enumerate(old)
        )

    def advance(b, g):
        at = pl.ds(pl.multiple_of(b * LANES, LANES), LANES)
        terms, new = advance_block(g, record[:, at], shares[:, at], steam, count_s[b])
        next_record[:, at] = new
        return tuple(zip(*(three_parts(t) for t in terms)))

    def hot(offset):
        return jnp.where(spot == offset[0:1], 1.0, 0.0).astype(jnp.bfloat16)

    zero = jnp.zeros((8, LANES), F32)

    def group(i, _):
        base = i * UNROLL
        spans = []
        for u in range(UNROLL):
            first = cell_s[(base + u) * LANES] // LANES
            last = cell_s[(base + u) * LANES + LANES - 1] // LANES
            spans.append((first, last))
        narrow = functools.reduce(
            jnp.logical_and, [last - first < WIDE for first, last in spans]
        )

        @pl.when(narrow)
        def _():
            staged = []
            for u in range(UNROLL):
                first = spans[u][0]
                tile_of, offset = prepare(base + u)
                g = (zero, zero)
                for j in range(WIDE):
                    g = pick(gas[first + j], tile_of, offset, first, j, g)
                staged.append((first, tile_of, offset, g))
            staged = [
                (first, tile_of, offset, advance(base + u, g))
                for u, (first, tile_of, offset, g) in enumerate(staged)
            ]
            for first, tile_of, offset, parts in staged:
                deposit(parts, tile_of, first, hot(offset), WIDE, acc)

        @pl.when(jnp.logical_not(narrow))
        def _():
            def one(u, _):
                b = base + u
                first = cell_s[b * LANES] // LANES
                last = cell_s[b * LANES + LANES - 1] // LANES
                tile_of, offset = prepare(b)

                def step(t, g):
                    return pick(gas[t], tile_of, offset, t, 0, g)

                g = lax.fori_loop(first, last + 1, step, (zero, zero))
                parts = advance(b, g)
                onehot = hot(offset)

                def put(t, _):
                    deposit(parts, tile_of, t, onehot, 1, acc)
                    return 0

                return lax.fori_loop(first, last + 1, put, 0)

            lax.fori_loop(0, UNROLL, one, 0)

        return 0

    lax.fori_loop(0, blocks // UNROLL, group, 0)

    for k in range(per_plane):
        low, high = acc[k], acc[per_plane + inner + k]
        send_a[k] = jnp.where(even, high, low)
        send_b[k] = jnp.where(even, low, high)

    planes = inner // per_plane
    lane = lax.broadcasted_iota(jnp.int32, (8, LANES), 1)
    take = lax.rem(lane * 2, LANES)
    row = lax.broadcasted_iota(jnp.int32, (1, 16, 1), 1)

    def mass_of(stack):
        return jnp.sum(jnp.where(row < species, stack, 0.0), axis=1) * (1.0 / volume_inverse)

    def halves(pick_tiles):
        out = []
        for k in range(per_plane):
            mass = mass_of(pick_tiles(k))
            both = mass + pltpu.roll(mass, LANES - 1, axis=1)
            out.append(jnp.take_along_axis(both, take, axis=1))
        return [
            jnp.where(lane < LANES // 2, out[2 * i], out[2 * i + 1])
            for i in range(per_plane // 2)
        ]

    own = halves(
        lambda k: jnp.stack([acc[(p + 1) * per_plane + k] for p in range(planes)])
    )
    for i, piece in enumerate(own):
        coarse[:, i * LANES : (i + 1) * LANES] = piece
    ends = halves(
        lambda k: jnp.stack([acc[k], acc[per_plane + inner + k]] + [jnp.zeros((16, LANES), F32)] * 6)
    )
    columns = per_plane // 2 * LANES
    quarter = per_plane // 8
    for h in range(2):
        for i, piece in enumerate(ends):
            r, c = 4 * h + i // quarter, i % quarter
            coarse[r : r + 1, columns + c * LANES : columns + (c + 1) * LANES] = piece[h : h + 1]


def merge_kernel(acc, pair_a, pair_b, out):
    fields, planes, cells = out.shape
    per_plane = cells // LANES
    even = plane_sides()
    for k in range(per_plane):
        a, b = pair_a[k], pair_b[k]
        from_above = jnp.where(even, a, b)
        from_below = jnp.where(even, b, a)
        rows = [acc[(p + 1) * per_plane + k] for p in range(planes)]
        rows[0] = rows[0] + from_below
        rows[planes - 1] = rows[planes - 1] + from_above
        x = jnp.swapaxes(jnp.stack(rows), 0, 1)
        x = jnp.concatenate([x[fields - 4 :], x[: fields - 4]], axis=0)
        out[:, :, k * LANES : (k + 1) * LANES] = x


def relax_kernel(masks, columns, *refs):
    *parts, out, source, one, two = refs
    planes = parts[0].shape[1]
    cross_count = lax.axis_size("cross")
    slab_count = lax.axis_size("slab")
    me = lax.axis_index("slab") * cross_count + lax.axis_index("cross")
    edge = COARSE
    slabs = edge // planes
    pieces = [(mask, part, i) for part, part_masks in zip(parts, masks) for i, mask in enumerate(part_masks)]

    def place(mask):
        owner = lax.bitwise_xor(me, mask)
        slab = owner // cross_count
        at = pl.multiple_of(lax.rem(owner, cross_count) * columns, LANES)
        return slab, at

    for mask, part, i in pieces:
        slab, at = place(mask)
        source[slab, :, pl.ds(at, columns)] = part[i, :, :columns]
    quarter = columns // 4
    for mask, part, i in pieces:
        slab, at = place(mask)
        for h, target, line in ((0, slab - 1, planes - 1), (1, slab + 1, 0)):
            @pl.when((target >= 0) & (target < slab_count))
            def _():
                for j in range(4):
                    here = pl.ds(pl.multiple_of(at + j * quarter, LANES), quarter)
                    r = 4 * h + j
                    source[target, line : line + 1, here] = (
                        source[target, line : line + 1, here] + part[i, r : r + 1, columns:]
                    )

    squared = edge * edge
    width = squared // LANES
    lane = lax.broadcasted_iota(jnp.int32, (8, LANES), 1)
    row = lax.broadcasted_iota(jnp.int32, (8, LANES), 0)
    inside = lax.rem(lane, edge)
    sixth = 1.0 / 6.0

    def at_lanes(v):
        return pl.ds(v * LANES, LANES)

    def sweep(src, dst):
        def run(s, _):
            up = jnp.minimum(s + 1, slabs - 1)
            dn = jnp.maximum(s - 1, 0)
            has_up = s < slabs - 1
            has_dn = s > 0
            values = [src[s, :, at_lanes(v)] for v in range(width)]
            turned = [pltpu.roll(x, edge, axis=1) for x in values]
            for v in range(width):
                x = values[v]
                above = src[up, 0:1, at_lanes(v)]
                under = src[dn, 7:8, at_lanes(v)]
                above = jnp.where(has_up, above, 0.0)
                under = jnp.where(has_dn, under, 0.0)
                total = jnp.where(row == 7, above, pltpu.roll(x, 7, axis=0))
                total = total + jnp.where(row == 0, under, pltpu.roll(x, 1, axis=0))
                left = turned[v - 1] if v > 0 else jnp.zeros_like(x)
                right = turned[v + 1] if v < width - 1 else jnp.zeros_like(x)
                total = total + turned[v] + jnp.where(lane < edge, left, right)
                total = total + jnp.where(inside < edge - 1, pltpu.roll(x, LANES - 1, axis=1), 0.0)
                total = total + jnp.where(inside > 0, pltpu.roll(x, 1, axis=1), 0.0)
                dst(s, v, (total + source[s, :, at_lanes(v)]) * sixth)
            return 0

        lax.fori_loop(0, slabs, run, 0)

    def into(ref):
        def put(s, v, x):
            ref[s, :, at_lanes(v)] = x
        return put

    def final(s, v, x):
        out[pl.ds(pl.multiple_of(s * 8, 8), 8), at_lanes(v)] = x

    def begin(s, _):
        one[s] = source[s] * sixth
        return 0

    lax.fori_loop(0, slabs, begin, 0)
    buffers = (one, two)
    for step in range(1, SWEEPS):
        src = buffers[(step - 1) % 2]
        sweep(src, final if step == SWEEPS - 1 else into(buffers[step % 2]))


def neighbour_pairs(slab_count, cross_count, start):
    pairs = []
    for s in range(start, slab_count - 1, 2):
        for c in range(cross_count):
            i, j = s * cross_count + c, (s + 1) * cross_count + c
            pairs += [(i, j), (j, i)]
    return pairs


def body(gas_state, parcel_record, condensed_shares, surface_steam_factor, fine_cell, block_counts):
    fields, planes, cells = gas_state.shape
    slots = parcel_record.shape[1]
    slab_count = lax.axis_size("slab")
    cross_count = lax.axis_size("cross")
    device_count = slab_count * cross_count
    squared = COARSE * COARSE
    fine_per_coarse = planes * slab_count // COARSE
    columns = cells * cross_count // squared
    columns = cells // columns
    per_plane = cells // LANES
    inner = planes * per_plane
    blocks = slots // BLOCK
    pairs_a = neighbour_pairs(slab_count, cross_count, 0)
    pairs_b = neighbour_pairs(slab_count, cross_count, 1)

    def swap(a, b):
        return lax.ppermute(a, AXES, pairs_a), lax.ppermute(b, AXES, pairs_b)

    plane = jax.ShapeDtypeStruct((per_plane, fields, LANES), F32)
    edge_a, edge_b = pl.pallas_call(
        edges_kernel, out_shape=(plane, plane), in_specs=[VMEM], out_specs=(VMEM, VMEM), name="edges"
    )(gas_state)
    got_a, got_b = swap(edge_a, edge_b)
    tiles = pl.pallas_call(
        tiles_kernel,
        out_shape=jax.ShapeDtypeStruct((inner, fields, LANES), F32),
        in_specs=[VMEM], out_specs=VMEM, name="tiles",
    )(gas_state)
    total_tiles = inner + 2 * per_plane + WIDE
    parcel_next, acc, send_a, send_b, coarse = pl.pallas_call(
        parcels_kernel,
        out_shape=(
            jax.ShapeDtypeStruct(parcel_record.shape, F32),
            jax.ShapeDtypeStruct((total_tiles, fields, LANES), F32),
            plane,
            plane,
            jax.ShapeDtypeStruct((8, columns + columns // 4), F32),
        ),
        in_specs=[SMEM, SMEM, SMEM] + [VMEM] * 6,
        out_specs=(VMEM,) * 5,
        scratch_shapes=[pltpu.VMEM((total_tiles, fields, LANES), F32)],
        name="parcels",
    )(
        fine_cell, block_counts, surface_steam_factor, fine_cell.reshape(blocks, LANES),
        tiles, got_a, got_b, parcel_record, condensed_shares,
    )
    back_a, back_b = swap(send_a, send_b)
    fine_source = pl.pallas_call(
        merge_kernel,
        out_shape=jax.ShapeDtypeStruct(gas_state.shape, F32),
        in_specs=[VMEM] * 3, out_specs=VMEM, name="merge",
    )(acc, back_a, back_b)

    own_planes = planes
    if fine_per_coarse != 1:
        coarse, own_planes = shared_planes(coarse, columns, planes, fine_per_coarse)
    parts, masks = gather_all(coarse, device_count)
    if fine_per_coarse == 1:
        scratch = pltpu.VMEM((COARSE // planes, planes, squared), F32)
        correction = pl.pallas_call(
            functools.partial(relax_kernel, masks, columns),
            out_shape=jax.ShapeDtypeStruct((COARSE, squared), F32),
            in_specs=[VMEM] * len(parts), out_specs=VMEM,
            scratch_shapes=[scratch] * 3, name="relax",
        )(*parts)
    else:
        correction = relax_plain(arrange(parts, masks, columns, own_planes, fine_per_coarse, planes))
    return (parcel_next, fine_source, correction)


def gather_all(x, device_count):
    bits = list(range(device_count.bit_length() - 1))[::-1]
    groups = []
    upper = bits[:-1]
    if len(upper) % 2:
        groups.append(upper[:1])
        upper = upper[1:]
    groups += [upper[i : i + 2] for i in range(0, len(upper), 2)]
    held, masks = x[None], [0]

    def send(mask):
        return lax.ppermute(held, AXES, [(i, i ^ mask) for i in range(device_count)])

    for group in groups:
        steps = [1 << group[0]]
        if len(group) == 2:
            steps += [1 << group[1], (1 << group[0]) + (1 << group[1])]
        arrived = [send(mask) for mask in steps]
        held = jnp.concatenate([held] + arrived, axis=0)
        masks = masks + [m ^ mask for mask in steps for m in masks]
    return (held, send(1)), (masks, [m ^ 1 for m in masks])


def shared_planes(coarse, columns, planes, fine_per_coarse):
    slab_count = lax.axis_size("slab")
    slab_index = lax.axis_index("slab")
    own = coarse[:, :columns]
    ends = coarse[:, columns:].reshape(2, columns)
    up = [(i, i + 1) for i in range(slab_count - 1)]
    down = [(j, i) for i, j in up]
    own = own.at[planes - 1].add(lax.ppermute(ends[0], "slab", down))
    own = own.at[0].add(lax.ppermute(ends[1], "slab", up))
    if fine_per_coarse <= planes:
        own = own.reshape(planes // fine_per_coarse, fine_per_coarse, columns).sum(axis=1)
        return own.reshape(-1, LANES), planes // fine_per_coarse
    own = own.sum(axis=0)
    group = fine_per_coarse // planes
    for level in range(group.bit_length() - 2, -1, -1):
        half = own.shape[0] // 2
        upper_side = slab_index // 2**level % 2 == 1
        keep = jnp.where(upper_side, own[half:], own[:half])
        send = jnp.where(upper_side, own[:half], own[half:])
        pairs = [(i, i ^ 1 << level) for i in range(slab_count)]
        own = keep + lax.ppermute(send, "slab", pairs)
    return own.reshape(-1, LANES), 1


def arrange(parts, masks, columns, own_planes, fine_per_coarse, planes):
    slab_count = lax.axis_size("slab")
    cross_count = lax.axis_size("cross")
    me = lax.axis_index("slab") * cross_count + lax.axis_index("cross")
    rows = jnp.concatenate(parts, axis=0)
    rows = rows.reshape(rows.shape[0], -1)
    distance = jnp.array([m for part in masks for m in part], jnp.int32)
    position = jnp.argsort(distance)[lax.bitwise_xor(me, jnp.arange(rows.shape[0]))]
    rows = rows[position]
    if fine_per_coarse <= planes:
        rows = rows.reshape(slab_count, cross_count, own_planes, columns)
    else:
        group = fine_per_coarse // planes
        rows = rows.reshape(COARSE, group, cross_count, columns // group)
    return jnp.transpose(rows, (0, 2, 1, 3)).reshape(COARSE, COARSE * COARSE)


def neighbours(grid):
    edge = grid.shape[0]
    x = jnp.pad(grid, ((1, 1), (0, 0)))
    y = jnp.pad(grid, ((0, 0), (edge, edge)))
    z = jnp.pad(grid, ((0, 0), (1, 1)))
    depth = jnp.arange(grid.shape[1], dtype=jnp.int32) % edge
    total = x[2:] + x[:-2] + y[:, 2 * edge :] + y[:, : -2 * edge]
    return total + jnp.where(depth < edge - 1, z[:, 2:], 0.0) + jnp.where(depth > 0, z[:, :-2], 0.0)


def relax_plain(coarse_source):
    correction = jnp.zeros_like(coarse_source)
    for _ in range(SWEEPS):
        correction = (neighbours(correction) + coarse_source) / 6.0
    return correction


def solution(mesh):
    in_specs = (
        P(None, "slab", "cross"),
        P(None, ("slab", "cross")),
        P(None, ("slab", "cross")),
        P(),
        P(("slab", "cross")),
        P(("slab", "cross")),
    )
    out_specs = (P(None, ("slab", "cross")), P(None, "slab", "cross"), P())
    return jax.shard_map(body, mesh=mesh, in_specs=in_specs, out_specs=out_specs, check_vma=False)
```

```python
import functools

import jax
import jax.numpy as jnp
from jax import lax
from jax.experimental import pallas as pl
from jax.experimental.pallas import tpu as pltpu
from jax.sharding import PartitionSpec as P

BLOCK = 128
COARSE = 64
SWEEPS = 4
LANES = 128
WIDE = 8
UNROLL = 4
AXES = ("slab", "cross")
F32 = jnp.float32
VMEM = pl.BlockSpec(memory_space=pltpu.VMEM)
SMEM = pl.BlockSpec(memory_space=pltpu.SMEM)


def room(mib):
    return pltpu.CompilerParams(vmem_limit_bytes=mib * 2**20)


drag_rate = 0.5
evap_rate = 0.08
warming_speed = 0.3
latent_boiling_energy = 0.5
vapour_heat = 1.5
volume_inverse = 4.0


def rows_in(tile, species):
    return jnp.concatenate([tile[:, 4 : 4 + species], tile[:, 0:4]], axis=1)


def plane_sides():
    return lax.rem(lax.axis_index("slab"), 2) == 0


def edges_kernel(gas, first_pair, second_pair):
    fields, planes, cells = gas.shape
    even = plane_sides()
    for k in range(cells // LANES):
        x = jnp.swapaxes(gas[:, :, k * LANES : (k + 1) * LANES], 0, 1)
        low, high = (rows_in(x[p : p + 1], fields - 4)[0] for p in (0, planes - 1))
        first_pair[k] = jnp.where(even, high, low)
        second_pair[k] = jnp.where(even, low, high)


def tiles_kernel(gas, tiles):
    fields, planes, cells = gas.shape
    per_plane = cells // LANES
    for k in range(per_plane):
        x = jnp.swapaxes(gas[:, :, k * LANES : (k + 1) * LANES], 0, 1)
        x = rows_in(x, fields - 4)
        for p in range(planes):
            tiles[p * per_plane + k] = x[p]


def advance_block(g, record, shares, steam, count):
    species = shares.shape[0]
    lane = lax.broadcasted_iota(jnp.int32, (1, LANES), 1)
    row = lax.broadcasted_iota(jnp.int32, (8, LANES), 0)
    rest = species - 8
    zeros = jnp.zeros((8 - rest, LANES), F32)
    g0, g1 = g
    s0 = shares[0:8]
    s1 = jnp.concatenate([shares[8:species], zeros], axis=0)
    r = jnp.concatenate([zeros, record[0:4]], axis=0)
    thermal = record[3:4]
    mass = record[4:5]
    d = g1 - r
    moving = (row >= 4) & (row < 7)
    slip_squared = jnp.sum(jnp.where(moving, d * d, 0.0), axis=0, keepdims=True)
    log_mass = jnp.log(mass)
    drag = (
        drag_rate
        * jnp.exp(log_mass * (-2.0 / 3.0))
        * (1.0 + 0.15 * jnp.exp(0.3435 * jnp.log(slip_squared + 1.0)))
    )
    following = (r + drag * g1) / (1.0 + drag)
    vapour = jnp.exp(2.0 * (thermal - 0.75))
    scale = evap_rate * mass
    rate0 = scale * (s0 * steam[0:8] * vapour - g0)
    rate1 = scale * (s1 * steam[8:16] * vapour - g1)
    evap = jnp.sum(rate0 + jnp.where(row < rest, rate1, 0.0), axis=0, keepdims=True)
    heat = warming_speed * d[7:8] * jnp.exp(log_mass * (1.0 / 3.0))
    next_thermal = thermal + (heat - latent_boiling_energy * evap) / mass
    next_mass = mass - evap
    momentum = mass * (r - following) + evap * following
    energy = vapour_heat * evap - heat
    alive = lane < count
    weight = jnp.where(alive, volume_inverse, 0.0)
    terms0 = rate0 * weight
    terms1 = jnp.where(row < rest, rate1, jnp.where(row < 7, momentum, energy)) * weight
    updated = jnp.concatenate([following[4:7], next_thermal, next_mass], axis=0)
    return (terms0, terms1), jnp.where(alive, updated, record)


def three_parts(x):
    high = x.astype(jnp.bfloat16).astype(F32)
    x = x - high
    middle = x.astype(jnp.bfloat16).astype(F32)
    return high, middle, x - middle


def deposit(parts, tile_of, first, onehot, number, acc):
    stack = []
    for j in range(number):
        here = tile_of == first + j
        for t0, t1 in parts:
            both = jnp.concatenate([jnp.where(here, t0, 0.0), jnp.where(here, t1, 0.0)], axis=0)
            stack.append(both.astype(jnp.bfloat16))
    stack = jnp.concatenate(stack, axis=0)
    sums = lax.dot_general(
        stack, onehot, (((1,), (1,)), ((), ())), preferred_element_type=F32
    )
    rows = 16
    for j in range(number):
        base = j * len(parts) * rows
        total = sums[base : base + rows]
        for i in range(1, len(parts)):
            total = total + sums[base + i * rows : base + (i + 1) * rows]
        acc[first + j] = acc[first + j] + total


def parcels_kernel(
    cell_s, count_s, steam_s, cell_v, tiles, pair_a, pair_b, record, shares,
    next_record, acc, send_a, send_b, coarse, gas,
):
    per_plane = pair_a.shape[0]
    inner = tiles.shape[0]
    blocks = cell_v.shape[0]
    species = shares.shape[0]
    even = plane_sides()
    below = jnp.where(even, 1, 0)
    for k in range(per_plane):
        a, b = pair_a[k], pair_b[k]
        gas[k] = jnp.where(even, b, a)
        gas[per_plane + inner + k] = jnp.where(even, a, b)

    def fill(i, _):
        for u in range(8):
            gas[per_plane + i * 8 + u] = tiles[i * 8 + u]
        return 0

    lax.fori_loop(0, inner // 8, fill, 0)

    def clear(i, _):
        for u in range(8):
            acc[i * 8 + u] = jnp.zeros(acc.shape[1:], F32)
        return 0

    lax.fori_loop(0, acc.shape[0] // 8, clear, 0)

    species_row = lax.broadcasted_iota(jnp.int32, (16, 1), 0)
    steam = jnp.zeros((16, 1), F32)
    for j in range(species):
        steam = jnp.where(species_row == j, steam_s[j], steam)
    steam = jnp.broadcast_to(steam, (16, LANES))
    spot = lax.broadcasted_iota(jnp.int32, (LANES, LANES), 0)

    def prepare(b):
        cell = cell_v[pl.ds(b, 1), :]
        return cell // LANES, jnp.broadcast_to(lax.rem(cell, LANES), (8, LANES))

    def pick(tile, tile_of, offset, first, j, old):
        here = tile_of == first + j
        return tuple(
            jnp.where(here, jnp.take_along_axis(tile[h * 8 : h * 8 + 8], offset, axis=1), o)
            for h, o in enumerate(old)
        )

    def advance(b, g):
        at = pl.ds(pl.multiple_of(b * LANES, LANES), LANES)
        terms, new = advance_block(g, record[:, at], shares[:, at], steam, count_s[b])
        next_record[:, at] = new
        return tuple(zip(*(three_parts(t) for t in terms)))

    def hot(offset):
        return jnp.where(spot == offset[0:1], 1.0, 0.0).astype(jnp.bfloat16)

    zero = jnp.zeros((8, LANES), F32)

    def group(i, _):
        base = i * UNROLL
        spans = []
        for u in range(UNROLL):
            first = cell_s[(base + u) * LANES] // LANES
            last = cell_s[(base + u) * LANES + LANES - 1] // LANES
            spans.append((first, last))
        narrow = functools.reduce(
            jnp.logical_and, [last - first < WIDE for first, last in spans]
        )

        @pl.when(narrow)
        def _():
            staged = []
            for u in range(UNROLL):
                first = spans[u][0]
                tile_of, offset = prepare(base + u)
                g = (zero, zero)
                for j in range(WIDE):
                    g = pick(gas[first + j], tile_of, offset, first, j, g)
                staged.append((first, tile_of, offset, g))
            staged = [
                (first, tile_of, offset, advance(base + u, g))
                for u, (first, tile_of, offset, g) in enumerate(staged)
            ]
            for first, tile_of, offset, parts in staged:
                deposit(parts, tile_of, first, hot(offset), WIDE, acc)

        @pl.when(jnp.logical_not(narrow))
        def _():
            def one(u, _):
                b = base + u
                first = cell_s[b * LANES] // LANES
                last = cell_s[b * LANES + LANES - 1] // LANES
                tile_of, offset = prepare(b)

                def step(t, g):
                    return pick(gas[t], tile_of, offset, t, 0, g)

                g = lax.fori_loop(first, last + 1, step, (zero, zero))
                parts = advance(b, g)
                onehot = hot(offset)

                def put(t, _):
                    deposit(parts, tile_of, t, onehot, 1, acc)
                    return 0

                return lax.fori_loop(first, last + 1, put, 0)

            lax.fori_loop(0, UNROLL, one, 0)

        return 0

    lax.fori_loop(0, blocks // UNROLL, group, 0)

    for k in range(per_plane):
        low, high = acc[k], acc[per_plane + inner + k]
        send_a[k] = jnp.where(even, high, low)
        send_b[k] = jnp.where(even, low, high)

    planes = inner // per_plane
    lane = lax.broadcasted_iota(jnp.int32, (8, LANES), 1)
    take = lax.rem(lane * 2, LANES)
    row = lax.broadcasted_iota(jnp.int32, (1, 16, 1), 1)

    def mass_of(stack):
        return jnp.sum(jnp.where(row < species, stack, 0.0), axis=1) * (1.0 / volume_inverse)

    def halves(pick_tiles):
        out = []
        for k in range(per_plane):
            mass = mass_of(pick_tiles(k))
            both = mass + pltpu.roll(mass, LANES - 1, axis=1)
            out.append(jnp.take_along_axis(both, take, axis=1))
        return [
            jnp.where(lane < LANES // 2, out[2 * i], out[2 * i + 1])
            for i in range(per_plane // 2)
        ]

    own = halves(
        lambda k: jnp.stack([acc[(p + 1) * per_plane + k] for p in range(planes)])
    )
    for i, piece in enumerate(own):
        coarse[:, i * LANES : (i + 1) * LANES] = piece
    ends = halves(
        lambda k: jnp.stack([acc[k], acc[per_plane + inner + k]] + [jnp.zeros((16, LANES), F32)] * 6)
    )
    columns = per_plane // 2 * LANES
    quarter = per_plane // 8
    for h in range(2):
        for i, piece in enumerate(ends):
            r, c = 4 * h + i // quarter, i % quarter
            coarse[r : r + 1, columns + c * LANES : columns + (c + 1) * LANES] = piece[h : h + 1]


def merge_kernel(acc, pair_a, pair_b, out):
    fields, planes, cells = out.shape
    per_plane = cells // LANES
    even = plane_sides()
    for k in range(per_plane):
        a, b = pair_a[k], pair_b[k]
        from_above = jnp.where(even, a, b)
        from_below = jnp.where(even, b, a)
        rows = [acc[(p + 1) * per_plane + k] for p in range(planes)]
        rows[0] = rows[0] + from_below
        rows[planes - 1] = rows[planes - 1] + from_above
        x = jnp.swapaxes(jnp.stack(rows), 0, 1)
        x = jnp.concatenate([x[fields - 4 :], x[: fields - 4]], axis=0)
        out[:, :, k * LANES : (k + 1) * LANES] = x


def relax_kernel(masks, columns, *refs):
    *parts, out, source, ends, one, two = refs
    planes = parts[0].shape[1]
    cross_count = lax.axis_size("cross")
    me = lax.axis_index("slab") * cross_count + lax.axis_index("cross")
    edge = COARSE
    slabs = edge // planes
    quarter = columns // 4
    squared = edge * edge
    width = squared // LANES
    lane = lax.broadcasted_iota(jnp.int32, (8, LANES), 1)
    row = lax.broadcasted_iota(jnp.int32, (8, LANES), 0)
    inside = lax.rem(lane, edge)
    sixth = 1.0 / 6.0

    for i in (0, slabs + 1):
        ends[i] = jnp.zeros(ends.shape[1:], F32)
        one[i] = jnp.zeros(one.shape[1:], F32)
        two[i] = jnp.zeros(two.shape[1:], F32)
    for part, part_masks in zip(parts, masks):
        for i, mask in enumerate(part_masks):
            owner = lax.bitwise_xor(me, mask)
            slab = owner // cross_count
            cross = lax.rem(owner, cross_count)
            at = pl.ds(pl.multiple_of(cross * columns, LANES), columns)
            source[slab, :, at] = part[i, :, :columns]
            at = pl.ds(pl.multiple_of(cross * quarter, LANES), quarter)
            ends[slab + 1, :, at] = part[i, :, columns:]

    def at_lanes(v):
        return pl.ds(v * LANES, LANES)

    def begin(s, _):
        for v in range(width):
            j, l = v * LANES % columns // quarter, v * LANES % quarter
            here = pl.ds(v * LANES // columns * quarter + l, LANES)
            above = jnp.broadcast_to(ends[s + 2, j : j + 1, here], (8, LANES))
            under = jnp.broadcast_to(ends[s, 4 + j : 5 + j, here], (8, LANES))
            x = source[s, :, at_lanes(v)]
            x = x + jnp.where(row == 7, above, jnp.where(row == 0, under, 0.0))
            source[s, :, at_lanes(v)] = x
            one[s + 1, :, at_lanes(v)] = x * sixth
        return 0

    lax.fori_loop(0, slabs, begin, 0)

    def sweep(src, put):
        def run(s, _):
            nothing = jnp.zeros((8, LANES), F32)
            x, turned = nothing, nothing
            after = src[s + 1, :, at_lanes(0)]
            turned_after = pltpu.roll(after, edge, axis=1)
            for v in range(width):
                turned_before = turned
                x, turned = after, turned_after
                if v < width - 1:
                    after = src[s + 1, :, at_lanes(v + 1)]
                    turned_after = pltpu.roll(after, edge, axis=1)
                else:
                    turned_after = nothing
                above = jnp.broadcast_to(src[s + 2, 0:1, at_lanes(v)], (8, LANES))
                under = jnp.broadcast_to(src[s, 7:8, at_lanes(v)], (8, LANES))
                total = source[s, :, at_lanes(v)] + turned
                total = total + jnp.where(lane < edge, turned_before, turned_after)
                total = total + jnp.where(row == 7, above, pltpu.roll(x, 7, axis=0))
                total = total + jnp.where(row == 0, under, pltpu.roll(x, 1, axis=0))
                total = total + jnp.where(inside < edge - 1, pltpu.roll(x, LANES - 1, axis=1), 0.0)
                total = total + jnp.where(inside > 0, pltpu.roll(x, 1, axis=1), 0.0)
                put(s, v, total * sixth)
            return 0

        lax.fori_loop(0, slabs, run, 0)

    def into(ref):
        def put(s, v, x):
            ref[s + 1, :, at_lanes(v)] = x
        return put

    def final(s, v, x):
        out[pl.ds(pl.multiple_of(s * 8, 8), 8), at_lanes(v)] = x

    buffers = (one, two)
    for step in range(1, SWEEPS):
        src = buffers[(step - 1) % 2]
        sweep(src, final if step == SWEEPS - 1 else into(buffers[step % 2]))


def neighbour_pairs(slab_count, cross_count, start):
    pairs = []
    for s in range(start, slab_count - 1, 2):
        for c in range(cross_count):
            i, j = s * cross_count + c, (s + 1) * cross_count + c
            pairs += [(i, j), (j, i)]
    return pairs


def body(gas_state, parcel_record, condensed_shares, surface_steam_factor, fine_cell, block_counts):
    fields, planes, cells = gas_state.shape
    slots = parcel_record.shape[1]
    slab_count = lax.axis_size("slab")
    cross_count = lax.axis_size("cross")
    device_count = slab_count * cross_count
    squared = COARSE * COARSE
    fine_per_coarse = planes * slab_count // COARSE
    columns = cells * cross_count // squared
    columns = cells // columns
    per_plane = cells // LANES
    inner = planes * per_plane
    blocks = slots // BLOCK
    pairs_a = neighbour_pairs(slab_count, cross_count, 0)
    pairs_b = neighbour_pairs(slab_count, cross_count, 1)

    def swap(a, b):
        return lax.ppermute(a, AXES, pairs_a), lax.ppermute(b, AXES, pairs_b)

    plane = jax.ShapeDtypeStruct((per_plane, fields, LANES), F32)
    edge_a, edge_b = pl.pallas_call(
        edges_kernel, out_shape=(plane, plane), in_specs=[VMEM], out_specs=(VMEM, VMEM), name="edges", compiler_params=room(8)
    )(gas_state)
    got_a, got_b = swap(edge_a, edge_b)
    tiles = pl.pallas_call(
        tiles_kernel,
        out_shape=jax.ShapeDtypeStruct((inner, fields, LANES), F32),
        in_specs=[VMEM], out_specs=VMEM, name="tiles", compiler_params=room(8),
    )(gas_state)
    total_tiles = inner + 2 * per_plane + WIDE
    parcel_next, acc, send_a, send_b, coarse = pl.pallas_call(
        parcels_kernel,
        out_shape=(
            jax.ShapeDtypeStruct(parcel_record.shape, F32),
            jax.ShapeDtypeStruct((total_tiles, fields, LANES), F32),
            plane,
            plane,
            jax.ShapeDtypeStruct((8, columns + columns // 4), F32),
        ),
        in_specs=[SMEM, SMEM, SMEM] + [VMEM] * 6,
        out_specs=(VMEM,) * 5,
        scratch_shapes=[pltpu.VMEM((total_tiles, fields, LANES), F32)],
        name="parcels", compiler_params=room(16),
    )(
        fine_cell, block_counts, surface_steam_factor, fine_cell.reshape(blocks, LANES),
        tiles, got_a, got_b, parcel_record, condensed_shares,
    )
    back_a, back_b = swap(send_a, send_b)
    fine_source = pl.pallas_call(
        merge_kernel,
        out_shape=jax.ShapeDtypeStruct(gas_state.shape, F32),
        in_specs=[VMEM] * 3, out_specs=VMEM, name="merge", compiler_params=room(12),
    )(acc, back_a, back_b)

    own_planes = planes
    if fine_per_coarse != 1:
        coarse, own_planes = shared_planes(coarse, columns, planes, fine_per_coarse)
    parts, masks = gather_all(coarse, device_count)
    if fine_per_coarse == 1:
        slabs = COARSE // planes
        padded = pltpu.VMEM((slabs + 2, planes, squared), F32)
        correction = pl.pallas_call(
            functools.partial(relax_kernel, masks, columns),
            out_shape=jax.ShapeDtypeStruct((COARSE, squared), F32),
            in_specs=[VMEM] * len(parts), out_specs=VMEM,
            scratch_shapes=[
                pltpu.VMEM((slabs, planes, squared), F32),
                pltpu.VMEM((slabs + 2, 8, squared // 4), F32),
                padded,
                padded,
            ],
            name="relax", compiler_params=room(16),
        )(*parts)
    else:
        correction = relax_plain(arrange(parts, masks, columns, own_planes, fine_per_coarse, planes))
    return (parcel_next, fine_source, correction)


def gather_all(x, device_count):
    bits = list(range(device_count.bit_length() - 1))[::-1]
    groups = []
    upper = bits[:-1]
    if len(upper) % 2:
        groups.append(upper[:1])
        upper = upper[1:]
    groups += [upper[i : i + 2] for i in range(0, len(upper), 2)]
    held, masks = x[None], [0]

    def send(mask):
        return lax.ppermute(held, AXES, [(i, i ^ mask) for i in range(device_count)])

    for group in groups:
        steps = [1 << group[0]]
        if len(group) == 2:
            steps += [1 << group[1], (1 << group[0]) + (1 << group[1])]
        arrived = [send(mask) for mask in steps]
        held = jnp.concatenate([held] + arrived, axis=0)
        masks = masks + [m ^ mask for mask in steps for m in masks]
    return (held, send(1)), (masks, [m ^ 1 for m in masks])


def shared_planes(coarse, columns, planes, fine_per_coarse):
    slab_count = lax.axis_size("slab")
    slab_index = lax.axis_index("slab")
    own = coarse[:, :columns]
    ends = coarse[:, columns:].reshape(2, columns)
    up = [(i, i + 1) for i in range(slab_count - 1)]
    down = [(j, i) for i, j in up]
    own = own.at[planes - 1].add(lax.ppermute(ends[0], "slab", down))
    own = own.at[0].add(lax.ppermute(ends[1], "slab", up))
    if fine_per_coarse <= planes:
        own = own.reshape(planes // fine_per_coarse, fine_per_coarse, columns).sum(axis=1)
        return own.reshape(-1, LANES), planes // fine_per_coarse
    own = own.sum(axis=0)
    group = fine_per_coarse // planes
    for level in range(group.bit_length() - 2, -1, -1):
        half = own.shape[0] // 2
        upper_side = slab_index // 2**level % 2 == 1
        keep = jnp.where(upper_side, own[half:], own[:half])
        send = jnp.where(upper_side, own[:half], own[half:])
        pairs = [(i, i ^ 1 << level) for i in range(slab_count)]
        own = keep + lax.ppermute(send, "slab", pairs)
    return own.reshape(-1, LANES), 1


def arrange(parts, masks, columns, own_planes, fine_per_coarse, planes):
    slab_count = lax.axis_size("slab")
    cross_count = lax.axis_size("cross")
    me = lax.axis_index("slab") * cross_count + lax.axis_index("cross")
    rows = jnp.concatenate(parts, axis=0)
    rows = rows.reshape(rows.shape[0], -1)
    distance = jnp.array([m for part in masks for m in part], jnp.int32)
    position = jnp.argsort(distance)[lax.bitwise_xor(me, jnp.arange(rows.shape[0]))]
    rows = rows[position]
    if fine_per_coarse <= planes:
        rows = rows.reshape(slab_count, cross_count, own_planes, columns)
    else:
        group = fine_per_coarse // planes
        rows = rows.reshape(COARSE, group, cross_count, columns // group)
    return jnp.transpose(rows, (0, 2, 1, 3)).reshape(COARSE, COARSE * COARSE)


def neighbours(grid):
    edge = grid.shape[0]
    x = jnp.pad(grid, ((1, 1), (0, 0)))
    y = jnp.pad(grid, ((0, 0), (edge, edge)))
    z = jnp.pad(grid, ((0, 0), (1, 1)))
    depth = jnp.arange(grid.shape[1], dtype=jnp.int32) % edge
    total = x[2:] + x[:-2] + y[:, 2 * edge :] + y[:, : -2 * edge]
    return total + jnp.where(depth < edge - 1, z[:, 2:], 0.0) + jnp.where(depth > 0, z[:, :-2], 0.0)


def relax_plain(coarse_source):
    correction = jnp.zeros_like(coarse_source)
    for _ in range(SWEEPS):
        correction = (neighbours(correction) + coarse_source) / 6.0
    return correction


def solution(mesh):
    in_specs = (
        P(None, "slab", "cross"),
        P(None, ("slab", "cross")),
        P(None, ("slab", "cross")),
        P(),
        P(("slab", "cross")),
        P(("slab", "cross")),
    )
    out_specs = (P(None, ("slab", "cross")), P(None, "slab", "cross"), P())
    return jax.shard_map(body, mesh=mesh, in_specs=in_specs, out_specs=out_specs, check_vma=False)
```

```python
import functools

import jax
import jax.numpy as jnp
from jax import lax
from jax.experimental import pallas as pl
from jax.experimental.pallas import tpu as pltpu
from jax.sharding import PartitionSpec as P


BLOCK = 128
COARSE = 64
SWEEPS = 4
LANES = 128
WIDE = 8
UNROLL = 4
AXES = ("slab", "cross")
F32 = jnp.float32
VMEM = pl.BlockSpec(memory_space=pltpu.VMEM)
SMEM = pl.BlockSpec(memory_space=pltpu.SMEM)
HBM = pl.BlockSpec(memory_space=pltpu.HBM)


def room(mib):
    return pltpu.CompilerParams(vmem_limit_bytes=mib * 2**20)


drag_rate = 0.5
evap_rate = 0.08
warming_speed = 0.3
latent_boiling_energy = 0.5
vapour_heat = 1.5
volume_inverse = 4.0


def rows_in(tile, species):
    return jnp.concatenate([tile[:, 4 : 4 + species], tile[:, 0:4]], axis=1)


def plane_sides():
    return lax.rem(lax.axis_index("slab"), 2) == 0


def load_kernel(
    gas_in, record_in, shares_in, rows_in_hbm, count_in, steam_in,
    gas, record, shares, rows, count, steam, first_pair, second_pair, sems,
):
    copies = [
        pltpu.make_async_copy(source, target, sems.at[i])
        for i, (source, target) in enumerate(
            [
                (gas_in, gas), (record_in, record), (shares_in, shares),
                (rows_in_hbm, rows), (count_in, count), (steam_in, steam),
            ]
        )
    ]
    for copy in copies:
        copy.start()
    fields, planes, cells = gas.shape
    even = plane_sides()
    copies[0].wait()
    for k in range(cells // LANES):
        x = jnp.swapaxes(gas[:, :, k * LANES : (k + 1) * LANES], 0, 1)
        low, high = (rows_in(x[p : p + 1], fields - 4)[0] for p in (0, planes - 1))
        first_pair[k] = jnp.where(even, high, low)
        second_pair[k] = jnp.where(even, low, high)
    for copy in copies[1:]:
        copy.wait()


def advance_block(g, record, shares, steam, count):
    species = shares.shape[0]
    lane = lax.broadcasted_iota(jnp.int32, (1, LANES), 1)
    row = lax.broadcasted_iota(jnp.int32, (8, LANES), 0)
    rest = species - 8
    zeros = jnp.zeros((8 - rest, LANES), F32)
    g0, g1 = g
    s0 = shares[0:8]
    s1 = jnp.concatenate([shares[8:species], zeros], axis=0)
    r = jnp.concatenate([zeros, record[0:4]], axis=0)
    thermal = record[3:4]
    mass = record[4:5]
    d = g1 - r
    moving = (row >= 4) & (row < 7)
    slip_squared = jnp.sum(jnp.where(moving, d * d, 0.0), axis=0, keepdims=True)
    log_mass = jnp.log(mass)
    drag = (
        drag_rate
        * jnp.exp(log_mass * (-2.0 / 3.0))
        * (1.0 + 0.15 * jnp.exp(0.3435 * jnp.log(slip_squared + 1.0)))
    )
    following = (r + drag * g1) / (1.0 + drag)
    vapour = jnp.exp(2.0 * (thermal - 0.75))
    scale = evap_rate * mass
    rate0 = scale * (s0 * steam[0:8] * vapour - g0)
    rate1 = scale * (s1 * steam[8:16] * vapour - g1)
    evap = jnp.sum(rate0 + jnp.where(row < rest, rate1, 0.0), axis=0, keepdims=True)
    heat = warming_speed * d[7:8] * jnp.exp(log_mass * (1.0 / 3.0))
    next_thermal = thermal + (heat - latent_boiling_energy * evap) / mass
    next_mass = mass - evap
    momentum = mass * (r - following) + evap * following
    energy = vapour_heat * evap - heat
    alive = lane < count
    weight = jnp.where(alive, volume_inverse, 0.0)
    terms0 = rate0 * weight
    terms1 = jnp.where(row < rest, rate1, jnp.where(row < 7, momentum, energy)) * weight
    updated = jnp.concatenate([following[4:7], next_thermal, next_mass], axis=0)
    return (terms0, terms1), jnp.where(alive, updated, record)


def three_parts(x):
    high = x.astype(jnp.bfloat16).astype(F32)
    x = x - high
    middle = x.astype(jnp.bfloat16).astype(F32)
    return high, middle, x - middle


def deposit(parts, tile_of, first, onehot, number, acc):
    stack = []
    for j in range(number):
        here = tile_of == first + j
        for t0, t1 in parts:
            both = jnp.concatenate([jnp.where(here, t0, 0.0), jnp.where(here, t1, 0.0)], axis=0)
            stack.append(both.astype(jnp.bfloat16))
    stack = jnp.concatenate(stack, axis=0)
    sums = lax.dot_general(
        stack, onehot, (((1,), (1,)), ((), ())), preferred_element_type=F32
    )
    rows = 16
    for j in range(number):
        base = j * len(parts) * rows
        total = sums[base : base + rows]
        for i in range(1, len(parts)):
            total = total + sums[base + i * rows : base + (i + 1) * rows]
        acc[first + j] = acc[first + j] + total


def run_groups(wanted, scalar_s, steam_s, cell_v, record, shares, next_record, acc, gas):
    blocks = cell_v.shape[0]
    species = shares.shape[0]
    species_row = lax.broadcasted_iota(jnp.int32, (16, 1), 0)
    steam = jnp.zeros((16, 1), F32)
    for j in range(species):
        steam = jnp.where(species_row == j, steam_s[j], steam)
    steam = jnp.broadcast_to(steam, (16, LANES))
    spot = lax.broadcasted_iota(jnp.int32, (LANES, LANES), 0)
    zero = jnp.zeros((8, LANES), F32)

    def prepare(b):
        cell = cell_v[pl.ds(b, 1), :]
        return cell // LANES, jnp.broadcast_to(lax.rem(cell, LANES), (8, LANES))

    def pick(tile, tile_of, offset, number, old):
        here = tile_of == number
        return tuple(
            jnp.where(here, jnp.take_along_axis(tile[h * 8 : h * 8 + 8], offset, axis=1), o)
            for h, o in enumerate(old)
        )

    def advance(b, g):
        at = pl.ds(pl.multiple_of(b * LANES, LANES), LANES)
        terms, new = advance_block(g, record[:, at], shares[:, at], steam, scalar_s[2 * blocks + b])
        next_record[:, at] = new
        return tuple(zip(*(three_parts(t) for t in terms)))

    def hot(offset):
        return jnp.where(spot == offset[0:1], 1.0, 0.0).astype(jnp.bfloat16)

    def span(b):
        return scalar_s[b], scalar_s[blocks + b]

    def group(i, _):
        base = i * UNROLL
        spans = [span(base + u) for u in range(UNROLL)]
        chosen = wanted(spans[0][0], spans[-1][1])
        narrow = functools.reduce(
            jnp.logical_and, [last - first < WIDE for first, last in spans]
        )

        @pl.when(chosen & narrow)
        def _():
            staged = []
            for u in range(UNROLL):
                first = spans[u][0]
                tile_of, offset = prepare(base + u)
                g = (zero, zero)
                for j in range(WIDE):
                    g = pick(gas[first + j], tile_of, offset, first + j, g)
                staged.append((first, tile_of, offset, g))
            staged = [
                (first, tile_of, offset, advance(base + u, g))
                for u, (first, tile_of, offset, g) in enumerate(staged)
            ]
            for first, tile_of, offset, parts in staged:
                deposit(parts, tile_of, first, hot(offset), WIDE, acc)

        @pl.when(chosen & jnp.logical_not(narrow))
        def _():
            def one(u, _):
                b = base + u
                first, last = span(b)
                tile_of, offset = prepare(b)

                def step(t, g):
                    return pick(gas[t], tile_of, offset, t, g)

                g = lax.fori_loop(first, last + 1, step, (zero, zero))
                parts = advance(b, g)
                onehot = hot(offset)

                def put(t, _):
                    deposit(parts, tile_of, t, onehot, 1, acc)
                    return 0

                return lax.fori_loop(first, last + 1, put, 0)

            lax.fori_loop(0, UNROLL, one, 0)

        return 0

    lax.fori_loop(0, blocks // UNROLL, group, 0)


def inside_planes(per_plane, inner):
    return lambda first, last: (first >= per_plane) & (last < per_plane + inner)


def interior_kernel(
    scalar_s, steam_s, cell_v, gas_state, record, shares, next_record, acc, gas
):
    fields, planes, cells = gas_state.shape
    per_plane = cells // LANES
    inner = planes * per_plane

    def clear(i, _):
        for u in range(8):
            acc[i * 8 + u] = jnp.zeros(acc.shape[1:], F32)
        return 0

    lax.fori_loop(0, acc.shape[0] // 8, clear, 0)
    for k in range(per_plane):
        x = jnp.swapaxes(gas_state[:, :, k * LANES : (k + 1) * LANES], 0, 1)
        x = rows_in(x, fields - 4)
        for p in range(planes):
            gas[(p + 1) * per_plane + k] = x[p]
    run_groups(
        inside_planes(per_plane, inner),
        scalar_s, steam_s, cell_v, record, shares, next_record, acc, gas,
    )


def border_kernel(
    scalar_s, steam_s, cell_v, pair_a, pair_b, record, shares,
    record_before, acc_before, gas_before, next_record, acc, send_a, send_b, coarse, gas,
):
    per_plane = pair_a.shape[0]
    inner = acc.shape[0] - 2 * per_plane - WIDE
    next_record[...] = record_before[...]

    def carry(i, _):
        for u in range(8):
            acc[i * 8 + u] = acc_before[i * 8 + u]
            gas[i * 8 + u] = gas_before[i * 8 + u]
        return 0

    lax.fori_loop(0, acc.shape[0] // 8, carry, 0)
    species = shares.shape[0]
    even = plane_sides()
    for k in range(per_plane):
        a, b = pair_a[k], pair_b[k]
        gas[k] = jnp.where(even, b, a)
        gas[per_plane + inner + k] = jnp.where(even, a, b)
    within = inside_planes(per_plane, inner)
    run_groups(
        lambda first, last: jnp.logical_not(within(first, last)),
        scalar_s, steam_s, cell_v, record, shares, next_record, acc, gas,
    )
    for k in range(per_plane):
        low, high = acc[k], acc[per_plane + inner + k]
        send_a[k] = jnp.where(even, high, low)
        send_b[k] = jnp.where(even, low, high)

    planes = inner // per_plane
    lane = lax.broadcasted_iota(jnp.int32, (8, LANES), 1)
    take = lax.rem(lane * 2, LANES)
    row = lax.broadcasted_iota(jnp.int32, (1, 16, 1), 1)

    def mass_of(stack):
        return jnp.sum(jnp.where(row < species, stack, 0.0), axis=1) * (1.0 / volume_inverse)

    def halves(pick_tiles):
        out = []
        for k in range(per_plane):
            mass = mass_of(pick_tiles(k))
            both = mass + pltpu.roll(mass, LANES - 1, axis=1)
            out.append(jnp.take_along_axis(both, take, axis=1))
        return [
            jnp.where(lane < LANES // 2, out[2 * i], out[2 * i + 1])
            for i in range(per_plane // 2)
        ]

    own = halves(
        lambda k: jnp.stack([acc[(p + 1) * per_plane + k] for p in range(planes)])
    )
    for i, piece in enumerate(own):
        coarse[:, i * LANES : (i + 1) * LANES] = piece
    ends = halves(
        lambda k: jnp.stack([acc[k], acc[per_plane + inner + k]] + [jnp.zeros((16, LANES), F32)] * 6)
    )
    columns = per_plane // 2 * LANES
    quarter = per_plane // 8
    for h in range(2):
        for i, piece in enumerate(ends):
            r, c = 4 * h + i // quarter, i % quarter
            coarse[r : r + 1, columns + c * LANES : columns + (c + 1) * LANES] = piece[h : h + 1]


def merge_kernel(acc, pair_a, pair_b, out):
    fields, planes, cells = out.shape
    per_plane = cells // LANES
    even = plane_sides()
    for k in range(per_plane):
        a, b = pair_a[k], pair_b[k]
        from_above = jnp.where(even, a, b)
        from_below = jnp.where(even, b, a)
        rows = [acc[(p + 1) * per_plane + k] for p in range(planes)]
        rows[0] = rows[0] + from_below
        rows[planes - 1] = rows[planes - 1] + from_above
        x = jnp.swapaxes(jnp.stack(rows), 0, 1)
        x = jnp.concatenate([x[fields - 4 :], x[: fields - 4]], axis=0)
        out[:, :, k * LANES : (k + 1) * LANES] = x


def relax_kernel(masks, columns, *refs):
    *parts, out, source, ends, one, two, done, sems = refs
    planes = parts[0].shape[1]
    cross_count = lax.axis_size("cross")
    me = lax.axis_index("slab") * cross_count + lax.axis_index("cross")
    edge = COARSE
    slabs = edge // planes
    quarter = columns // 4
    squared = edge * edge
    width = squared // LANES
    lane = lax.broadcasted_iota(jnp.int32, (8, LANES), 1)
    row = lax.broadcasted_iota(jnp.int32, (8, LANES), 0)
    inside = lax.rem(lane, edge)
    sixth = 1.0 / 6.0

    for i in (0, slabs + 1):
        ends[i] = jnp.zeros(ends.shape[1:], F32)
        one[i] = jnp.zeros(one.shape[1:], F32)
        two[i] = jnp.zeros(two.shape[1:], F32)
    for part, part_masks in zip(parts, masks):
        for i, mask in enumerate(part_masks):
            owner = lax.bitwise_xor(me, mask)
            slab = owner // cross_count
            cross = lax.rem(owner, cross_count)
            at = pl.ds(pl.multiple_of(cross * columns, LANES), columns)
            source[slab, :, at] = part[i, :, :columns]
            at = pl.ds(pl.multiple_of(cross * quarter, LANES), quarter)
            ends[slab + 1, :, at] = part[i, :, columns:]

    def at_lanes(v):
        return pl.ds(v * LANES, LANES)

    def begin(s, _):
        for v in range(width):
            j, l = v * LANES % columns // quarter, v * LANES % quarter
            here = pl.ds(v * LANES // columns * quarter + l, LANES)
            above = jnp.broadcast_to(ends[s + 2, j : j + 1, here], (8, LANES))
            under = jnp.broadcast_to(ends[s, 4 + j : 5 + j, here], (8, LANES))
            x = source[s, :, at_lanes(v)]
            x = x + jnp.where(row == 7, above, jnp.where(row == 0, under, 0.0))
            source[s, :, at_lanes(v)] = x
            one[s + 1, :, at_lanes(v)] = x * sixth
        return 0

    lax.fori_loop(0, slabs, begin, 0)

    def sweep(src, put):
        def run(s, _):
            nothing = jnp.zeros((8, LANES), F32)
            x, turned = nothing, nothing
            after = src[s + 1, :, at_lanes(0)]
            turned_after = pltpu.roll(after, edge, axis=1)
            for v in range(width):
                turned_before = turned
                x, turned = after, turned_after
                if v < width - 1:
                    after = src[s + 1, :, at_lanes(v + 1)]
                    turned_after = pltpu.roll(after, edge, axis=1)
                else:
                    turned_after = nothing
                above = jnp.broadcast_to(src[s + 2, 0:1, at_lanes(v)], (8, LANES))
                under = jnp.broadcast_to(src[s, 7:8, at_lanes(v)], (8, LANES))
                total = source[s, :, at_lanes(v)] + turned
                total = total + jnp.where(lane < edge, turned_before, turned_after)
                total = total + jnp.where(row == 7, above, pltpu.roll(x, 7, axis=0))
                total = total + jnp.where(row == 0, under, pltpu.roll(x, 1, axis=0))
                total = total + jnp.where(inside < edge - 1, pltpu.roll(x, LANES - 1, axis=1), 0.0)
                total = total + jnp.where(inside > 0, pltpu.roll(x, 1, axis=1), 0.0)
                put(s, v, total * sixth)
            if put is final:
                leave(s).start()
            return 0

        lax.fori_loop(0, slabs, run, 0)

    def into(ref):
        def put(s, v, x):
            ref[s + 1, :, at_lanes(v)] = x

        return put

    def final(s, v, x):
        done[s, :, at_lanes(v)] = x

    def leave(s):
        rows = pl.ds(pl.multiple_of(s * 8, 8), 8)
        return pltpu.make_async_copy(done.at[s], out.at[rows], sems.at[s])

    buffers = (one, two)
    for step in range(1, SWEEPS):
        src = buffers[(step - 1) % 2]
        sweep(src, final if step == SWEEPS - 1 else into(buffers[step % 2]))
    for s in range(slabs):
        leave(s).wait()


def neighbour_pairs(slab_count, cross_count, start):
    pairs = []
    for s in range(start, slab_count - 1, 2):
        for c in range(cross_count):
            i, j = s * cross_count + c, (s + 1) * cross_count + c
            pairs += [(i, j), (j, i)]
    return pairs


def body(gas_state, parcel_record, condensed_shares, surface_steam_factor, fine_cell, block_counts):
    fields, planes, cells = gas_state.shape
    slots = parcel_record.shape[1]
    slab_count = lax.axis_size("slab")
    cross_count = lax.axis_size("cross")
    device_count = slab_count * cross_count
    squared = COARSE * COARSE
    fine_per_coarse = planes * slab_count // COARSE
    columns = cells * cross_count // squared
    columns = cells // columns
    per_plane = cells // LANES
    inner = planes * per_plane
    blocks = slots // BLOCK
    pairs_a = neighbour_pairs(slab_count, cross_count, 0)
    pairs_b = neighbour_pairs(slab_count, cross_count, 1)

    def swap(a, b):
        return lax.ppermute(a, AXES, pairs_a), lax.ppermute(b, AXES, pairs_b)

    plane = jax.ShapeDtypeStruct((per_plane, fields, LANES), F32)
    cell_rows = fine_cell.reshape(blocks, LANES)
    inputs = (
        gas_state, parcel_record, condensed_shares, cell_rows, block_counts, surface_steam_factor,
    )
    *held, edge_a, edge_b = pl.pallas_call(
        load_kernel,
        out_shape=tuple(jax.ShapeDtypeStruct(x.shape, x.dtype) for x in inputs) + (plane, plane),
        in_specs=[HBM] * 6, out_specs=(VMEM,) * 8,
        scratch_shapes=[pltpu.SemaphoreType.DMA((6,))],
        name="load", compiler_params=room(8),
    )(*[pltpu.with_memory_space_constraint(x, pltpu.HBM) for x in inputs])
    gas_state, parcel_record, condensed_shares, cell_rows, block_counts, steam = held
    got_a, got_b = swap(edge_a, edge_b)
    total_tiles = inner + 2 * per_plane + WIDE
    all_tiles = jax.ShapeDtypeStruct((total_tiles, fields, LANES), F32)
    record = jax.ShapeDtypeStruct(parcel_record.shape, F32)
    scalars = jnp.concatenate(
        [cell_rows[:, 0] // LANES, cell_rows[:, LANES - 1] // LANES, block_counts]
    )
    scalars = (scalars, steam)
    partial = pl.pallas_call(
        interior_kernel,
        out_shape=(record, all_tiles, all_tiles),
        in_specs=[SMEM] * 2 + [VMEM] * 4,
        out_specs=(VMEM,) * 3,
        name="interior", compiler_params=room(16),
    )(*scalars, cell_rows, gas_state, parcel_record, condensed_shares)
    parcel_next, acc, send_a, send_b, coarse = pl.pallas_call(
        border_kernel,
        out_shape=(
            record,
            all_tiles,
            plane,
            plane,
            jax.ShapeDtypeStruct((8, columns + columns // 4), F32),
        ),
        in_specs=[SMEM] * 2 + [VMEM] * 8,
        out_specs=(VMEM,) * 5,
        scratch_shapes=[pltpu.VMEM(all_tiles.shape, F32)],
        name="border", compiler_params=room(16),
    )(*scalars, cell_rows, got_a, got_b, parcel_record, condensed_shares, *partial)
    back_a, back_b = swap(send_a, send_b)
    fine_source = pl.pallas_call(
        merge_kernel,
        out_shape=jax.ShapeDtypeStruct(gas_state.shape, F32),
        in_specs=[VMEM] * 3, out_specs=VMEM, name="merge", compiler_params=room(12),
    )(acc, back_a, back_b)

    own_planes = planes
    if fine_per_coarse != 1:
        coarse, own_planes = shared_planes(coarse, columns, planes, fine_per_coarse)
    parts, masks = gather_all(coarse, device_count)
    if fine_per_coarse == 1:
        slabs = COARSE // planes
        padded = pltpu.VMEM((slabs + 2, planes, squared), F32)
        correction = pl.pallas_call(
            functools.partial(relax_kernel, masks, columns),
            out_shape=jax.ShapeDtypeStruct((COARSE, squared), F32),
            in_specs=[VMEM] * len(parts),
            out_specs=pl.BlockSpec(memory_space=pl.ANY),
            scratch_shapes=[
                pltpu.VMEM((slabs, planes, squared), F32),
                pltpu.VMEM((slabs + 2, 8, squared // 4), F32),
                padded,
                padded,
                pltpu.VMEM((slabs, planes, squared), F32),
                pltpu.SemaphoreType.DMA((slabs,)),
            ],
            name="relax", compiler_params=room(16),
        )(*parts)
    else:
        correction = relax_plain(arrange(parts, masks, columns, own_planes, fine_per_coarse, planes))
    return (parcel_next, fine_source, correction)


def gather_all(x, device_count):
    bits = list(range(device_count.bit_length() - 1))[::-1]
    groups = []
    upper = bits[:-1]
    if len(upper) % 2:
        groups.append(upper[:1])
        upper = upper[1:]
    groups += [upper[i : i + 2] for i in range(0, len(upper), 2)]
    held, masks = x[None], [0]

    def send(mask):
        return lax.ppermute(held, AXES, [(i, i ^ mask) for i in range(device_count)])

    for group in groups:
        steps = [1 << group[0]]
        if len(group) == 2:
            steps += [1 << group[1], (1 << group[0]) + (1 << group[1])]
        arrived = [send(mask) for mask in steps]
        held = jnp.concatenate([held] + arrived, axis=0)
        masks = masks + [m ^ mask for mask in steps for m in masks]
    other = send(1)
    return (held, other), (masks, [m ^ 1 for m in masks])


def shared_planes(coarse, columns, planes, fine_per_coarse):
    slab_count = lax.axis_size("slab")
    slab_index = lax.axis_index("slab")
    own = coarse[:, :columns]
    ends = coarse[:, columns:].reshape(2, columns)
    up = [(i, i + 1) for i in range(slab_count - 1)]
    down = [(j, i) for i, j in up]
    own = own.at[planes - 1].add(lax.ppermute(ends[0], "slab", down))
    own = own.at[0].add(lax.ppermute(ends[1], "slab", up))
    if fine_per_coarse <= planes:
        own = own.reshape(planes // fine_per_coarse, fine_per_coarse, columns).sum(axis=1)
        return own.reshape(-1, LANES), planes // fine_per_coarse
    own = own.sum(axis=0)
    group = fine_per_coarse // planes
    for level in range(group.bit_length() - 2, -1, -1):
        half = own.shape[0] // 2
        upper_side = slab_index // 2**level % 2 == 1
        keep = jnp.where(upper_side, own[half:], own[:half])
        send = jnp.where(upper_side, own[:half], own[half:])
        pairs = [(i, i ^ 1 << level) for i in range(slab_count)]
        own = keep + lax.ppermute(send, "slab", pairs)
    return own.reshape(-1, LANES), 1


def arrange(parts, masks, columns, own_planes, fine_per_coarse, planes):
    slab_count = lax.axis_size("slab")
    cross_count = lax.axis_size("cross")
    me = lax.axis_index("slab") * cross_count + lax.axis_index("cross")
    rows = jnp.concatenate(parts, axis=0)
    rows = rows.reshape(rows.shape[0], -1)
    distance = jnp.array([m for part in masks for m in part], jnp.int32)
    position = jnp.argsort(distance)[lax.bitwise_xor(me, jnp.arange(rows.shape[0]))]
    rows = rows[position]
    if fine_per_coarse <= planes:
        rows = rows.reshape(slab_count, cross_count, own_planes, columns)
    else:
        group = fine_per_coarse // planes
        rows = rows.reshape(COARSE, group, cross_count, columns // group)
    return jnp.transpose(rows, (0, 2, 1, 3)).reshape(COARSE, COARSE * COARSE)


def neighbours(grid):
    edge = grid.shape[0]
    x = jnp.pad(grid, ((1, 1), (0, 0)))
    y = jnp.pad(grid, ((0, 0), (edge, edge)))
    z = jnp.pad(grid, ((0, 0), (1, 1)))
    depth = jnp.arange(grid.shape[1], dtype=jnp.int32) % edge
    total = x[2:] + x[:-2] + y[:, 2 * edge :] + y[:, : -2 * edge]
    return total + jnp.where(depth < edge - 1, z[:, 2:], 0.0) + jnp.where(depth > 0, z[:, :-2], 0.0)


def relax_plain(coarse_source):
    correction = jnp.zeros_like(coarse_source)
    for _ in range(SWEEPS):
        correction = (neighbours(correction) + coarse_source) / 6.0
    return correction


def solution(mesh):
    in_specs = (
        P(None, "slab", "cross"),
        P(None, ("slab", "cross")),
        P(None, ("slab", "cross")),
        P(),
        P(("slab", "cross")),
        P(("slab", "cross")),
    )
    out_specs = (P(None, ("slab", "cross")), P(None, "slab", "cross"), P())

    def step(*args):
        return body(*args)

    step = jax.shard_map(step, mesh=mesh, in_specs=in_specs, out_specs=out_specs, check_vma=False)
    return step
```

```python
import functools

import jax
import jax.numpy as jnp
from jax import lax
from jax.experimental import pallas as pl
from jax.experimental.pallas import tpu as pltpu
from jax.sharding import PartitionSpec as P


BLOCK = 128
COARSE = 64
SWEEPS = 4
LANES = 128
WIDE = 8
UNROLL = 4
PIECES = 2
GROUP = 2
AXES = ("slab", "cross")
F32 = jnp.float32
VMEM = pl.BlockSpec(memory_space=pltpu.VMEM)
SMEM = pl.BlockSpec(memory_space=pltpu.SMEM)
HBM = pl.BlockSpec(memory_space=pltpu.HBM)


def room(mib):
    return pltpu.CompilerParams(vmem_limit_bytes=mib * 2**20)


drag_rate = 0.5
evap_rate = 0.08
warming_speed = 0.3
latent_boiling_energy = 0.5
vapour_heat = 1.5
volume_inverse = 4.0


def rows_in(tile, species):
    return jnp.concatenate([tile[:, 4 : 4 + species], tile[:, 0:4]], axis=1)


def plane_sides():
    return lax.rem(lax.axis_index("slab"), 2) == 0


def load_kernel(
    gas_in, record_in, shares_in, rows_in_hbm, count_in, steam_in,
    gas, record, shares, rows, count, steam, first_pair, second_pair, sems,
):
    fields, planes, cells = gas.shape
    step = fields // PIECES
    moves = [(gas_in.at[pl.ds(i * step, step)], gas.at[pl.ds(i * step, step)]) for i in range(PIECES)]
    moves += [
        (record_in, record), (shares_in, shares),
        (rows_in_hbm, rows), (count_in, count), (steam_in, steam),
    ]
    copies = [
        pltpu.make_async_copy(source, target, sems.at[i])
        for i, (source, target) in enumerate(moves)
    ]
    for copy in copies:
        copy.start()
    even = plane_sides()
    for copy in copies[:PIECES]:
        copy.wait()
    for k in range(cells // LANES):
        x = jnp.swapaxes(gas[:, :, k * LANES : (k + 1) * LANES], 0, 1)
        low, high = (rows_in(x[p : p + 1], fields - 4)[0] for p in (0, planes - 1))
        first_pair[k] = jnp.where(even, high, low)
        second_pair[k] = jnp.where(even, low, high)
    for copy in copies[PIECES:]:
        copy.wait()


def advance_block(g, record, shares, steam, count):
    species = shares.shape[0]
    lane = lax.broadcasted_iota(jnp.int32, (1, LANES), 1)
    row = lax.broadcasted_iota(jnp.int32, (8, LANES), 0)
    rest = species - 8
    zeros = jnp.zeros((8 - rest, LANES), F32)
    g0, g1 = g
    s0 = shares[0:8]
    s1 = jnp.concatenate([shares[8:species], zeros], axis=0)
    r = jnp.concatenate([zeros, record[0:4]], axis=0)
    thermal = record[3:4]
    mass = record[4:5]
    d = g1 - r
    moving = (row >= 4) & (row < 7)
    slip_squared = jnp.sum(jnp.where(moving, d * d, 0.0), axis=0, keepdims=True)
    log_mass = jnp.log(mass)
    drag = (
        drag_rate
        * jnp.exp(log_mass * (-2.0 / 3.0))
        * (1.0 + 0.15 * jnp.exp(0.3435 * jnp.log(slip_squared + 1.0)))
    )
    following = (r + drag * g1) / (1.0 + drag)
    vapour = jnp.exp(2.0 * (thermal - 0.75))
    scale = evap_rate * mass
    rate0 = scale * (s0 * steam[0:8] * vapour - g0)
    rate1 = scale * (s1 * steam[8:16] * vapour - g1)
    evap = jnp.sum(rate0 + jnp.where(row < rest, rate1, 0.0), axis=0, keepdims=True)
    heat = warming_speed * d[7:8] * jnp.exp(log_mass * (1.0 / 3.0))
    next_thermal = thermal + (heat - latent_boiling_energy * evap) / mass
    next_mass = mass - evap
    momentum = mass * (r - following) + evap * following
    energy = vapour_heat * evap - heat
    alive = lane < count
    weight = jnp.where(alive, volume_inverse, 0.0)
    terms0 = rate0 * weight
    terms1 = jnp.where(row < rest, rate1, jnp.where(row < 7, momentum, energy)) * weight
    updated = jnp.concatenate([following[4:7], next_thermal, next_mass], axis=0)
    return (terms0, terms1), jnp.where(alive, updated, record)


def three_parts(x):
    high = x.astype(jnp.bfloat16).astype(F32)
    x = x - high
    middle = x.astype(jnp.bfloat16).astype(F32)
    return high, middle, x - middle


def deposit(parts, tile_of, first, onehot, number, acc):
    stack = []
    for j in range(number):
        here = tile_of == first + j
        for t0, t1 in parts:
            both = jnp.concatenate([jnp.where(here, t0, 0.0), jnp.where(here, t1, 0.0)], axis=0)
            stack.append(both.astype(jnp.bfloat16))
    stack = jnp.concatenate(stack, axis=0)
    sums = lax.dot_general(
        stack, onehot, (((1,), (1,)), ((), ())), preferred_element_type=F32
    )
    rows = 16
    for j in range(number):
        base = j * len(parts) * rows
        total = sums[base : base + rows]
        for i in range(1, len(parts)):
            total = total + sums[base + i * rows : base + (i + 1) * rows]
        acc[first + j] = acc[first + j] + total


def run_groups(wanted, scalar_s, steam_s, cell_v, record, shares, next_record, acc, gas):
    blocks = cell_v.shape[0]
    species = shares.shape[0]
    species_row = lax.broadcasted_iota(jnp.int32, (16, 1), 0)
    steam = jnp.zeros((16, 1), F32)
    for j in range(species):
        steam = jnp.where(species_row == j, steam_s[j], steam)
    steam = jnp.broadcast_to(steam, (16, LANES))
    spot = lax.broadcasted_iota(jnp.int32, (LANES, LANES), 0)
    zero = jnp.zeros((8, LANES), F32)

    def prepare(b):
        cell = cell_v[pl.ds(b, 1), :]
        return cell // LANES, jnp.broadcast_to(lax.rem(cell, LANES), (8, LANES))

    def pick(tile, tile_of, offset, number, old):
        here = tile_of == number
        return tuple(
            jnp.where(here, jnp.take_along_axis(tile[h * 8 : h * 8 + 8], offset, axis=1), o)
            for h, o in enumerate(old)
        )

    def advance(b, g):
        at = pl.ds(pl.multiple_of(b * LANES, LANES), LANES)
        terms, new = advance_block(g, record[:, at], shares[:, at], steam, scalar_s[2 * blocks + b])
        next_record[:, at] = new
        return tuple(zip(*(three_parts(t) for t in terms)))

    def hot(offset):
        return jnp.where(spot == offset[0:1], 1.0, 0.0).astype(jnp.bfloat16)

    def span(b):
        return scalar_s[b], scalar_s[blocks + b]

    def group(i, _):
        base = i * UNROLL
        spans = [span(base + u) for u in range(UNROLL)]
        chosen = wanted(spans[0][0], spans[-1][1])
        narrow = functools.reduce(
            jnp.logical_and, [last - first < WIDE for first, last in spans]
        )

        @pl.when(chosen & narrow)
        def _():
            staged = []
            for u in range(UNROLL):
                first = spans[u][0]
                tile_of, offset = prepare(base + u)
                g = (zero, zero)
                for j in range(WIDE):
                    g = pick(gas(first + j), tile_of, offset, first + j, g)
                staged.append((first, tile_of, offset, g))
            staged = [
                (first, tile_of, offset, advance(base + u, g))
                for u, (first, tile_of, offset, g) in enumerate(staged)
            ]
            for first, tile_of, offset, parts in staged:
                deposit(parts, tile_of, first, hot(offset), WIDE, acc)

        @pl.when(chosen & jnp.logical_not(narrow))
        def _():
            def one(u, _):
                b = base + u
                first, last = span(b)
                tile_of, offset = prepare(b)

                def step(t, g):
                    return pick(gas(t), tile_of, offset, t, g)

                g = lax.fori_loop(first, last + 1, step, (zero, zero))
                parts = advance(b, g)
                onehot = hot(offset)

                def put(t, _):
                    deposit(parts, tile_of, t, onehot, 1, acc)
                    return 0

                return lax.fori_loop(first, last + 1, put, 0)

            lax.fori_loop(0, UNROLL, one, 0)

        return 0

    lax.fori_loop(0, blocks // UNROLL, group, 0)


def inside_planes(per_plane, inner):
    return lambda first, last: (first >= per_plane) & (last < per_plane + inner)


def interior_kernel(
    scalar_s, steam_s, cell_v, gas_state, record, shares, next_record, acc, gas
):
    fields, planes, cells = gas_state.shape
    per_plane = cells // LANES
    inner = planes * per_plane

    def clear(i, _):
        for u in range(8):
            acc[i * 8 + u] = jnp.zeros(acc.shape[1:], F32)
        return 0

    lax.fori_loop(0, acc.shape[0] // 8, clear, 0)
    for k in range(per_plane):
        x = jnp.swapaxes(gas_state[:, :, k * LANES : (k + 1) * LANES], 0, 1)
        x = rows_in(x, fields - 4)
        for p in range(planes):
            gas[(p + 1) * per_plane + k] = x[p]
    run_groups(
        inside_planes(per_plane, inner),
        scalar_s, steam_s, cell_v, record, shares, next_record, acc, lambda t: gas[t],
    )


def border_kernel(
    scalar_s, steam_s, cell_v, pair_a, pair_b, record, shares,
    record_before, acc_before, gas_before, next_record, acc, send_a, send_b, coarse, halo,
):
    per_plane = pair_a.shape[0]
    inner = acc.shape[0] - 2 * per_plane - WIDE
    next_record[...] = record_before[...]
    for i in range(0, acc.shape[0], 8):
        acc[i : i + 8] = acc_before[i : i + 8]
    species = shares.shape[0]
    even = plane_sides()
    for k in range(per_plane):
        a, b = pair_a[k], pair_b[k]
        halo[k] = jnp.where(even, b, a)
        halo[per_plane + k] = jnp.where(even, a, b)

    def gas(t):
        low = t < per_plane
        high = t >= per_plane + inner
        place = jnp.where(high, jnp.minimum(t - inner, 2 * per_plane - 1), jnp.minimum(t, per_plane - 1))
        return jnp.where(low | high, halo[place], gas_before[t])

    within = inside_planes(per_plane, inner)
    run_groups(
        lambda first, last: jnp.logical_not(within(first, last)),
        scalar_s, steam_s, cell_v, record, shares, next_record, acc, gas,
    )
    for k in range(per_plane):
        low, high = acc[k], acc[per_plane + inner + k]
        send_a[k] = jnp.where(even, high, low)
        send_b[k] = jnp.where(even, low, high)

    planes = inner // per_plane
    lane = lax.broadcasted_iota(jnp.int32, (8, LANES), 1)
    take = lax.rem(lane * 2, LANES)
    row = lax.broadcasted_iota(jnp.int32, (1, 16, 1), 1)

    def mass_of(stack):
        return jnp.sum(jnp.where(row < species, stack, 0.0), axis=1) * (1.0 / volume_inverse)

    def halves(pick_tiles):
        out = []
        for k in range(per_plane):
            mass = mass_of(pick_tiles(k))
            both = mass + pltpu.roll(mass, LANES - 1, axis=1)
            out.append(jnp.take_along_axis(both, take, axis=1))
        return [
            jnp.where(lane < LANES // 2, out[2 * i], out[2 * i + 1])
            for i in range(per_plane // 2)
        ]

    own = halves(
        lambda k: jnp.stack([acc[(p + 1) * per_plane + k] for p in range(planes)])
    )
    for i, piece in enumerate(own):
        coarse[:, i * LANES : (i + 1) * LANES] = piece
    ends = halves(
        lambda k: jnp.stack([acc[k], acc[per_plane + inner + k]] + [jnp.zeros((16, LANES), F32)] * 6)
    )
    columns = per_plane // 2 * LANES
    quarter = per_plane // 8
    for h in range(2):
        for i, piece in enumerate(ends):
            r, c = 4 * h + i // quarter, i % quarter
            coarse[r : r + 1, columns + c * LANES : columns + (c + 1) * LANES] = piece[h : h + 1]


def merge_kernel(acc, pair_a, pair_b, record_in, out, record):
    record[...] = record_in[...]
    fields, planes, cells = out.shape
    per_plane = cells // LANES
    even = plane_sides()
    for k in range(per_plane):
        a, b = pair_a[k], pair_b[k]
        from_above = jnp.where(even, a, b)
        from_below = jnp.where(even, b, a)
        rows = [acc[(p + 1) * per_plane + k] for p in range(planes)]
        rows[0] = rows[0] + from_below
        rows[planes - 1] = rows[planes - 1] + from_above
        x = jnp.swapaxes(jnp.stack(rows), 0, 1)
        x = jnp.concatenate([x[fields - 4 :], x[: fields - 4]], axis=0)
        out[:, :, k * LANES : (k + 1) * LANES] = x


def relax_kernel(masks, columns, *refs):
    *parts, out, source, ends, one, two, done, even_products, odd_products, sems = refs
    planes = parts[0].shape[1]
    cross_count = lax.axis_size("cross")
    me = lax.axis_index("slab") * cross_count + lax.axis_index("cross")
    edge = COARSE
    slabs = edge // planes
    quarter = columns // 4
    squared = edge * edge
    width = squared // LANES
    lane = lax.broadcasted_iota(jnp.int32, (8, LANES), 1)
    row = lax.broadcasted_iota(jnp.int32, (8, LANES), 0)
    sixth = 1.0 / 6.0

    pitch = width + 1

    def at_plane(plane, v):
        return pl.ds((plane + 1) * pitch + v, 8, stride=pitch)

    for i in (0, slabs + 1):
        ends[i] = jnp.zeros(ends.shape[1:], F32)
    for ref in (one, two):
        for start in (0, (edge + 1) * pitch):
            ref[pl.ds(start, pitch), :] = jnp.zeros((pitch, LANES), F32)
    for part, part_masks in zip(parts, masks):
        for i, mask in enumerate(part_masks):
            owner = lax.bitwise_xor(me, mask)
            slab = owner // cross_count
            cross = lax.rem(owner, cross_count)
            at = pl.ds(pl.multiple_of(cross * columns, LANES), columns)
            source[slab, :, at] = part[i, :, :columns]
            at = pl.ds(pl.multiple_of(cross * quarter, LANES), quarter)
            ends[slab + 1, :, at] = part[i, :, columns:]

    def at_lanes(v):
        return pl.ds(v * LANES, LANES)

    def begin(s, _):
        for v in range(width):
            j, l = v * LANES % columns // quarter, v * LANES % quarter
            here = pl.ds(v * LANES // columns * quarter + l, LANES)
            above = jnp.broadcast_to(ends[s + 2, j : j + 1, here], (8, LANES))
            under = jnp.broadcast_to(ends[s, 4 + j : 5 + j, here], (8, LANES))
            x = source[s, :, at_lanes(v)]
            x = x + jnp.where(row == 7, above, jnp.where(row == 0, under, 0.0))
            source[s, :, at_lanes(v)] = x
            one[at_plane(s * 8, v), :] = x * sixth
        return 0

    lax.fori_loop(0, slabs, begin, 0)

    k = lax.broadcasted_iota(jnp.int32, (2 * LANES, 2 * LANES), 0) % LANES
    l = lax.broadcasted_iota(jnp.int32, (2 * LANES, 2 * LANES), 1)
    crossed = k == lax.rem(l + edge, LANES)
    beside = (jnp.abs(k - l) == 1) & (k // edge == l // edge)
    near = jnp.where(crossed | beside, 1.0, 0.0).astype(jnp.bfloat16)

    def multiply(src, group, products):
        x = jnp.concatenate(
            [
                src[at_plane(s * 8, v), :]
                for s in range(group * GROUP, (group + 1) * GROUP)
                for v in range(width)
            ],
            axis=0,
        )
        high = x.astype(jnp.bfloat16)
        middle = (x - high.astype(F32)).astype(jnp.bfloat16)
        products[...] = jnp.dot(
            jnp.concatenate([high, middle], axis=1), near, preferred_element_type=F32
        )

    def combine(src, group, products, put):
        for i in range(GROUP):
            s = group * GROUP + i
            base = i * width * 8

            def turned(v):
                if 0 <= v < width:
                    return products[base + v * 8 : base + v * 8 + 8, LANES:]
                return jnp.zeros((8, LANES), F32)

            for v in range(width):
                total = source[s, :, at_lanes(v)] + products[base + v * 8 : base + v * 8 + 8, :LANES]
                total = total + jnp.where(lane < edge, turned(v - 1), turned(v + 1))
                total = total + src[at_plane(s * 8 + 1, v), :] + src[at_plane(s * 8 - 1, v), :]
                put(s, v, total * sixth)
            if put is final:
                leave(s).start()

    def sweep(src, put):
        groups = slabs // GROUP
        multiply(src, 0, even_products)
        for g in range(groups):
            now, later = (even_products, odd_products)[:: 1 if g % 2 == 0 else -1]
            if g + 1 < groups:
                multiply(src, g + 1, later)
            combine(src, g, now, put)

    def into(ref):
        def put(s, v, x):
            ref[at_plane(s * 8, v), :] = x

        return put

    def final(s, v, x):
        done[s, :, at_lanes(v)] = x

    def leave(s):
        rows = pl.ds(pl.multiple_of(s * 8, 8), 8)
        return pltpu.make_async_copy(done.at[s], out.at[rows], sems.at[s])

    buffers = (one, two)
    for step in range(1, SWEEPS):
        src = buffers[(step - 1) % 2]
        sweep(src, final if step == SWEEPS - 1 else into(buffers[step % 2]))
    for s in range(slabs):
        leave(s).wait()


def neighbour_pairs(slab_count, cross_count, start):
    pairs = []
    for s in range(start, slab_count - 1, 2):
        for c in range(cross_count):
            i, j = s * cross_count + c, (s + 1) * cross_count + c
            pairs += [(i, j), (j, i)]
    return pairs


def body(gas_state, parcel_record, condensed_shares, surface_steam_factor, fine_cell, block_counts):
    fields, planes, cells = gas_state.shape
    slots = parcel_record.shape[1]
    slab_count = lax.axis_size("slab")
    cross_count = lax.axis_size("cross")
    device_count = slab_count * cross_count
    squared = COARSE * COARSE
    fine_per_coarse = planes * slab_count // COARSE
    columns = cells * cross_count // squared
    columns = cells // columns
    per_plane = cells // LANES
    inner = planes * per_plane
    blocks = slots // BLOCK
    pairs_a = neighbour_pairs(slab_count, cross_count, 0)
    pairs_b = neighbour_pairs(slab_count, cross_count, 1)

    def swap(a, b):
        return lax.ppermute(a, AXES, pairs_a), lax.ppermute(b, AXES, pairs_b)

    plane = jax.ShapeDtypeStruct((per_plane, fields, LANES), F32)
    cell_rows = fine_cell.reshape(blocks, LANES)
    inputs = (
        gas_state, parcel_record, condensed_shares, cell_rows, block_counts, surface_steam_factor,
    )
    *held, edge_a, edge_b = pl.pallas_call(
        load_kernel,
        out_shape=tuple(jax.ShapeDtypeStruct(x.shape, x.dtype) for x in inputs) + (plane, plane),
        in_specs=[HBM] * 6, out_specs=(VMEM,) * 8,
        scratch_shapes=[pltpu.SemaphoreType.DMA((PIECES + 5,))],
        name="load", compiler_params=room(8),
    )(*[pltpu.with_memory_space_constraint(x, pltpu.HBM) for x in inputs])
    gas_state, parcel_record, condensed_shares, cell_rows, block_counts, steam = held
    got_a, got_b = swap(edge_a, edge_b)
    total_tiles = inner + 2 * per_plane + WIDE
    all_tiles = jax.ShapeDtypeStruct((total_tiles, fields, LANES), F32)
    record = jax.ShapeDtypeStruct(parcel_record.shape, F32)
    scalars = jnp.concatenate(
        [cell_rows[:, 0] // LANES, cell_rows[:, LANES - 1] // LANES, block_counts]
    )
    scalars = (scalars, steam)
    partial = pl.pallas_call(
        interior_kernel,
        out_shape=(record, all_tiles, all_tiles),
        in_specs=[SMEM] * 2 + [VMEM] * 4,
        out_specs=(VMEM,) * 3,
        name="interior", compiler_params=room(16),
    )(*scalars, cell_rows, gas_state, parcel_record, condensed_shares)
    updated, acc, send_a, send_b, coarse = pl.pallas_call(
        border_kernel,
        out_shape=(
            record,
            all_tiles,
            plane,
            plane,
            jax.ShapeDtypeStruct((8, columns + columns // 4), F32),
        ),
        in_specs=[SMEM] * 2 + [VMEM] * 8,
        out_specs=(VMEM,) * 5,
        scratch_shapes=[pltpu.VMEM((2 * per_plane, fields, LANES), F32)],
        name="border", compiler_params=room(16),
    )(*scalars, cell_rows, got_a, got_b, parcel_record, condensed_shares, *partial)
    back_a, back_b = swap(send_a, send_b)
    fine_source, parcel_next = pl.pallas_call(
        merge_kernel,
        out_shape=(jax.ShapeDtypeStruct(gas_state.shape, F32), record),
        in_specs=[VMEM] * 4, out_specs=(VMEM, VMEM), name="merge", compiler_params=room(12),
    )(acc, back_a, back_b, updated)

    own_planes = planes
    if fine_per_coarse != 1:
        coarse, own_planes = shared_planes(coarse, columns, planes, fine_per_coarse)
    parts, masks = gather_all(coarse, device_count)
    if fine_per_coarse == 1:
        slabs = COARSE // planes
        products = pltpu.VMEM((GROUP * planes * squared // LANES, 2 * LANES), F32)
        padded = pltpu.VMEM(((COARSE + 2) * (squared // LANES + 1), LANES), F32)
        correction = pl.pallas_call(
            functools.partial(relax_kernel, masks, columns),
            out_shape=jax.ShapeDtypeStruct((COARSE, squared), F32),
            in_specs=[VMEM] * len(parts),
            out_specs=pl.BlockSpec(memory_space=pl.ANY),
            scratch_shapes=[
                pltpu.VMEM((slabs, planes, squared), F32),
                pltpu.VMEM((slabs + 2, 8, squared // 4), F32),
                padded,
                padded,
                pltpu.VMEM((slabs, planes, squared), F32),
                products,
                products,
                pltpu.SemaphoreType.DMA((slabs,)),
            ],
            name="relax", compiler_params=room(16),
        )(*parts)
    else:
        correction = relax_plain(arrange(parts, masks, columns, own_planes, fine_per_coarse, planes))
    return (parcel_next, fine_source, correction)


def gather_all(x, device_count):
    bits = list(range(device_count.bit_length() - 1))[::-1]
    groups = []
    upper = bits[:-1]
    if len(upper) % 2:
        groups.append(upper[:1])
        upper = upper[1:]
    groups += [upper[i : i + 2] for i in range(0, len(upper), 2)]
    held, masks = x[None], [0]

    def send(mask):
        return lax.ppermute(held, AXES, [(i, i ^ mask) for i in range(device_count)])

    for group in groups:
        steps = [1 << group[0]]
        if len(group) == 2:
            steps += [1 << group[1], (1 << group[0]) + (1 << group[1])]
        arrived = []
        for mask in steps:
            arrived.append(send(mask))
        held = jnp.concatenate([held] + arrived, axis=0)
        masks = masks + [m ^ mask for mask in steps for m in masks]
    other = send(1)
    return (held, other), (masks, [m ^ 1 for m in masks])


def shared_planes(coarse, columns, planes, fine_per_coarse):
    slab_count = lax.axis_size("slab")
    slab_index = lax.axis_index("slab")
    own = coarse[:, :columns]
    ends = coarse[:, columns:].reshape(2, columns)
    up = [(i, i + 1) for i in range(slab_count - 1)]
    down = [(j, i) for i, j in up]
    own = own.at[planes - 1].add(lax.ppermute(ends[0], "slab", down))
    own = own.at[0].add(lax.ppermute(ends[1], "slab", up))
    if fine_per_coarse <= planes:
        own = own.reshape(planes // fine_per_coarse, fine_per_coarse, columns).sum(axis=1)
        return own.reshape(-1, LANES), planes // fine_per_coarse
    own = own.sum(axis=0)
    group = fine_per_coarse // planes
    for level in range(group.bit_length() - 2, -1, -1):
        half = own.shape[0] // 2
        upper_side = slab_index // 2**level % 2 == 1
        keep = jnp.where(upper_side, own[half:], own[:half])
        send = jnp.where(upper_side, own[:half], own[half:])
        pairs = [(i, i ^ 1 << level) for i in range(slab_count)]
        own = keep + lax.ppermute(send, "slab", pairs)
    return own.reshape(-1, LANES), 1


def arrange(parts, masks, columns, own_planes, fine_per_coarse, planes):
    slab_count = lax.axis_size("slab")
    cross_count = lax.axis_size("cross")
    me = lax.axis_index("slab") * cross_count + lax.axis_index("cross")
    rows = jnp.concatenate(parts, axis=0)
    rows = rows.reshape(rows.shape[0], -1)
    distance = jnp.array([m for part in masks for m in part], jnp.int32)
    position = jnp.argsort(distance)[lax.bitwise_xor(me, jnp.arange(rows.shape[0]))]
    rows = rows[position]
    if fine_per_coarse <= planes:
        rows = rows.reshape(slab_count, cross_count, own_planes, columns)
    else:
        group = fine_per_coarse // planes
        rows = rows.reshape(COARSE, group, cross_count, columns // group)
    return jnp.transpose(rows, (0, 2, 1, 3)).reshape(COARSE, COARSE * COARSE)


def neighbours(grid):
    edge = grid.shape[0]
    x = jnp.pad(grid, ((1, 1), (0, 0)))
    y = jnp.pad(grid, ((0, 0), (edge, edge)))
    z = jnp.pad(grid, ((0, 0), (1, 1)))
    depth = jnp.arange(grid.shape[1], dtype=jnp.int32) % edge
    total = x[2:] + x[:-2] + y[:, 2 * edge :] + y[:, : -2 * edge]
    return total + jnp.where(depth < edge - 1, z[:, 2:], 0.0) + jnp.where(depth > 0, z[:, :-2], 0.0)


def relax_plain(coarse_source):
    correction = jnp.zeros_like(coarse_source)
    for _ in range(SWEEPS):
        correction = (neighbours(correction) + coarse_source) / 6.0
    return correction


def solution(mesh):
    in_specs = (
        P(None, "slab", "cross"),
        P(None, ("slab", "cross")),
        P(None, ("slab", "cross")),
        P(),
        P(("slab", "cross")),
        P(("slab", "cross")),
    )
    out_specs = (P(None, ("slab", "cross")), P(None, "slab", "cross"), P())

    def step(*args):
        return body(*args)

    step = jax.shard_map(step, mesh=mesh, in_specs=in_specs, out_specs=out_specs, check_vma=False)
    return step
```

```python
import functools

import jax
import jax.numpy as jnp
from jax import lax
from jax.experimental import pallas as pl
from jax.experimental.pallas import tpu as pltpu
from jax.sharding import PartitionSpec as P


BLOCK = 128
COARSE = 64
SWEEPS = 4
LANES = 128
WIDE = 8
UNROLL = 4
PIECES = 2
GROUP = 2
AXES = ("slab", "cross")
F32 = jnp.float32
VMEM = pl.BlockSpec(memory_space=pltpu.VMEM)
SMEM = pl.BlockSpec(memory_space=pltpu.SMEM)
HBM = pl.BlockSpec(memory_space=pltpu.HBM)


def room(mib):
    return pltpu.CompilerParams(vmem_limit_bytes=mib * 2**20)


drag_rate = 0.5
evap_rate = 0.08
warming_speed = 0.3
latent_boiling_energy = 0.5
vapour_heat = 1.5
volume_inverse = 4.0


def rows_in(tile, species):
    return jnp.concatenate([tile[:, 4 : 4 + species], tile[:, 0:4]], axis=1)


def plane_sides():
    return lax.rem(lax.axis_index("slab"), 2) == 0


def load_kernel(
    gas_in, record_in, shares_in, rows_in_hbm, count_in, steam_in,
    gas, record, shares, rows, count, steam, first_pair, second_pair, sems,
):
    fields, planes, cells = gas.shape
    step = fields // PIECES
    moves = [(gas_in.at[pl.ds(i * step, step)], gas.at[pl.ds(i * step, step)]) for i in range(PIECES)]
    moves += [
        (record_in, record), (shares_in, shares),
        (rows_in_hbm, rows), (count_in, count), (steam_in, steam),
    ]
    copies = [
        pltpu.make_async_copy(source, target, sems.at[i])
        for i, (source, target) in enumerate(moves)
    ]
    for copy in copies:
        copy.start()
    even = plane_sides()
    for copy in copies[:PIECES]:
        copy.wait()
    for k in range(cells // LANES):
        x = jnp.swapaxes(gas[:, :, k * LANES : (k + 1) * LANES], 0, 1)
        low, high = (rows_in(x[p : p + 1], fields - 4)[0] for p in (0, planes - 1))
        first_pair[k] = jnp.where(even, high, low)
        second_pair[k] = jnp.where(even, low, high)
    for copy in copies[PIECES:]:
        copy.wait()


def advance_block(g, record, shares, steam, count):
    species = shares.shape[0]
    lane = lax.broadcasted_iota(jnp.int32, (1, LANES), 1)
    row = lax.broadcasted_iota(jnp.int32, (8, LANES), 0)
    rest = species - 8
    zeros = jnp.zeros((8 - rest, LANES), F32)
    g0, g1 = g
    s0 = shares[0:8]
    s1 = jnp.concatenate([shares[8:species], zeros], axis=0)
    r = jnp.concatenate([zeros, record[0:4]], axis=0)
    thermal = record[3:4]
    mass = record[4:5]
    d = g1 - r
    moving = (row >= 4) & (row < 7)
    slip_squared = jnp.sum(jnp.where(moving, d * d, 0.0), axis=0, keepdims=True)
    log_mass = jnp.log(mass)
    drag = (
        drag_rate
        * jnp.exp(log_mass * (-2.0 / 3.0))
        * (1.0 + 0.15 * jnp.exp(0.3435 * jnp.log(slip_squared + 1.0)))
    )
    following = (r + drag * g1) / (1.0 + drag)
    vapour = jnp.exp(2.0 * (thermal - 0.75))
    scale = evap_rate * mass
    rate0 = scale * (s0 * steam[0:8] * vapour - g0)
    rate1 = scale * (s1 * steam[8:16] * vapour - g1)
    evap = jnp.sum(rate0 + jnp.where(row < rest, rate1, 0.0), axis=0, keepdims=True)
    heat = warming_speed * d[7:8] * jnp.exp(log_mass * (1.0 / 3.0))
    next_thermal = thermal + (heat - latent_boiling_energy * evap) / mass
    next_mass = mass - evap
    momentum = mass * (r - following) + evap * following
    energy = vapour_heat * evap - heat
    alive = lane < count
    weight = jnp.where(alive, volume_inverse, 0.0)
    terms0 = rate0 * weight
    terms1 = jnp.where(row < rest, rate1, jnp.where(row < 7, momentum, energy)) * weight
    updated = jnp.concatenate([following[4:7], next_thermal, next_mass], axis=0)
    return (terms0, terms1), jnp.where(alive, updated, record)


def three_parts(x):
    high = x.astype(jnp.bfloat16).astype(F32)
    x = x - high
    middle = x.astype(jnp.bfloat16).astype(F32)
    return high, middle, x - middle


def deposit(parts, tile_of, first, onehot, number, acc):
    stack = []
    for j in range(number):
        here = tile_of == first + j
        for t0, t1 in parts:
            both = jnp.concatenate([jnp.where(here, t0, 0.0), jnp.where(here, t1, 0.0)], axis=0)
            stack.append(both.astype(jnp.bfloat16))
    stack = jnp.concatenate(stack, axis=0)
    sums = lax.dot_general(
        stack, onehot, (((1,), (1,)), ((), ())), preferred_element_type=F32
    )
    rows = 16
    for j in range(number):
        base = j * len(parts) * rows
        total = sums[base : base + rows]
        for i in range(1, len(parts)):
            total = total + sums[base + i * rows : base + (i + 1) * rows]
        acc[first + j] = acc[first + j] + total


def run_groups(wanted, scalar_s, steam_s, cell_v, record, shares, next_record, acc, gas):
    blocks = cell_v.shape[0]
    species = shares.shape[0]
    species_row = lax.broadcasted_iota(jnp.int32, (16, 1), 0)
    steam = jnp.zeros((16, 1), F32)
    for j in range(species):
        steam = jnp.where(species_row == j, steam_s[j], steam)
    steam = jnp.broadcast_to(steam, (16, LANES))
    spot = lax.broadcasted_iota(jnp.int32, (LANES, LANES), 0)
    zero = jnp.zeros((8, LANES), F32)

    def prepare(b):
        cell = cell_v[pl.ds(b, 1), :]
        return cell // LANES, jnp.broadcast_to(lax.rem(cell, LANES), (8, LANES))

    def pick(tile, tile_of, offset, number, old):
        here = tile_of == number
        return tuple(
            jnp.where(here, jnp.take_along_axis(tile[h * 8 : h * 8 + 8], offset, axis=1), o)
            for h, o in enumerate(old)
        )

    def advance(b, g):
        at = pl.ds(pl.multiple_of(b * LANES, LANES), LANES)
        terms, new = advance_block(g, record[:, at], shares[:, at], steam, scalar_s[2 * blocks + b])
        next_record[:, at] = new
        return tuple(zip(*(three_parts(t) for t in terms)))

    def hot(offset):
        return jnp.where(spot == offset[0:1], 1.0, 0.0).astype(jnp.bfloat16)

    def span(b):
        return scalar_s[b], scalar_s[blocks + b]

    def group(i, _):
        base = i * UNROLL
        spans = [span(base + u) for u in range(UNROLL)]
        chosen = wanted(spans[0][0], spans[-1][1])
        narrow = functools.reduce(
            jnp.logical_and, [last - first < WIDE for first, last in spans]
        )

        @pl.when(chosen & narrow)
        def _():
            staged = []
            for u in range(UNROLL):
                first = spans[u][0]
                tile_of, offset = prepare(base + u)
                g = (zero, zero)
                for j in range(WIDE):
                    g = pick(gas(first + j), tile_of, offset, first + j, g)
                staged.append((first, tile_of, offset, g))
            staged = [
                (first, tile_of, offset, advance(base + u, g))
                for u, (first, tile_of, offset, g) in enumerate(staged)
            ]
            for first, tile_of, offset, parts in staged:
                deposit(parts, tile_of, first, hot(offset), WIDE, acc)

        @pl.when(chosen & jnp.logical_not(narrow))
        def _():
            def one(u, _):
                b = base + u
                first, last = span(b)
                tile_of, offset = prepare(b)

                def step(t, g):
                    return pick(gas(t), tile_of, offset, t, g)

                g = lax.fori_loop(first, last + 1, step, (zero, zero))
                parts = advance(b, g)
                onehot = hot(offset)

                def put(t, _):
                    deposit(parts, tile_of, t, onehot, 1, acc)
                    return 0

                return lax.fori_loop(first, last + 1, put, 0)

            lax.fori_loop(0, UNROLL, one, 0)

        return 0

    lax.fori_loop(0, blocks // UNROLL, group, 0)


def inside_planes(per_plane, inner):
    return lambda first, last: (first >= per_plane) & (last < per_plane + inner)


def interior_kernel(
    scalar_s, steam_s, cell_v, gas_state, record, shares, next_record, acc, gas
):
    fields, planes, cells = gas_state.shape
    per_plane = cells // LANES
    inner = planes * per_plane

    def clear(i, _):
        for u in range(8):
            acc[i * 8 + u] = jnp.zeros(acc.shape[1:], F32)
        return 0

    lax.fori_loop(0, acc.shape[0] // 8, clear, 0)
    for k in range(per_plane):
        x = jnp.swapaxes(gas_state[:, :, k * LANES : (k + 1) * LANES], 0, 1)
        x = rows_in(x, fields - 4)
        for p in range(planes):
            gas[(p + 1) * per_plane + k] = x[p]
    run_groups(
        inside_planes(per_plane, inner),
        scalar_s, steam_s, cell_v, record, shares, next_record, acc, lambda t: gas[t],
    )


def border_kernel(
    scalar_s, steam_s, cell_v, pair_a, pair_b, record, shares,
    record_before, acc_before, gas_before, next_record, acc, send_a, send_b, coarse, halo,
):
    per_plane = pair_a.shape[0]
    inner = acc.shape[0] - 2 * per_plane - WIDE
    next_record[...] = record_before[...]
    for i in range(0, acc.shape[0], 8):
        acc[i : i + 8] = acc_before[i : i + 8]
    species = shares.shape[0]
    even = plane_sides()
    for k in range(per_plane):
        a, b = pair_a[k], pair_b[k]
        halo[k] = jnp.where(even, b, a)
        halo[per_plane + k] = jnp.where(even, a, b)

    def gas(t):
        low = t < per_plane
        high = t >= per_plane + inner
        place = jnp.where(high, jnp.minimum(t - inner, 2 * per_plane - 1), jnp.minimum(t, per_plane - 1))
        return jnp.where(low | high, halo[place], gas_before[t])

    within = inside_planes(per_plane, inner)
    run_groups(
        lambda first, last: jnp.logical_not(within(first, last)),
        scalar_s, steam_s, cell_v, record, shares, next_record, acc, gas,
    )
    for k in range(per_plane):
        low, high = acc[k], acc[per_plane + inner + k]
        send_a[k] = jnp.where(even, high, low)
        send_b[k] = jnp.where(even, low, high)

    planes = inner // per_plane
    lane = lax.broadcasted_iota(jnp.int32, (8, LANES), 1)
    take = lax.rem(lane * 2, LANES)
    row = lax.broadcasted_iota(jnp.int32, (1, 16, 1), 1)

    def mass_of(stack):
        return jnp.sum(jnp.where(row < species, stack, 0.0), axis=1) * (1.0 / volume_inverse)

    def halves(pick_tiles):
        out = []
        for k in range(per_plane):
            mass = mass_of(pick_tiles(k))
            both = mass + pltpu.roll(mass, LANES - 1, axis=1)
            out.append(jnp.take_along_axis(both, take, axis=1))
        return [
            jnp.where(lane < LANES // 2, out[2 * i], out[2 * i + 1])
            for i in range(per_plane // 2)
        ]

    own = halves(
        lambda k: jnp.stack([acc[(p + 1) * per_plane + k] for p in range(planes)])
    )
    for i, piece in enumerate(own):
        coarse[:, i * LANES : (i + 1) * LANES] = piece
    ends = halves(
        lambda k: jnp.stack([acc[k], acc[per_plane + inner + k]] + [jnp.zeros((16, LANES), F32)] * 6)
    )
    columns = per_plane // 2 * LANES
    quarter = per_plane // 8
    for h in range(2):
        for i, piece in enumerate(ends):
            r, c = 4 * h + i // quarter, i % quarter
            coarse[r : r + 1, columns + c * LANES : columns + (c + 1) * LANES] = piece[h : h + 1]


def merge_kernel(acc, pair_a, pair_b, record_in, out, record):
    record[...] = record_in[...]
    fields, planes, cells = out.shape
    per_plane = cells // LANES
    even = plane_sides()
    for k in range(per_plane):
        a, b = pair_a[k], pair_b[k]
        from_above = jnp.where(even, a, b)
        from_below = jnp.where(even, b, a)
        rows = [acc[(p + 1) * per_plane + k] for p in range(planes)]
        rows[0] = rows[0] + from_below
        rows[planes - 1] = rows[planes - 1] + from_above
        x = jnp.swapaxes(jnp.stack(rows), 0, 1)
        x = jnp.concatenate([x[fields - 4 :], x[: fields - 4]], axis=0)
        out[:, :, k * LANES : (k + 1) * LANES] = x


def relax_kernel(masks, columns, *refs):
    *parts, out, source, ends, one, two, done, even_products, odd_products, sems = refs
    planes = parts[0].shape[1]
    cross_count = lax.axis_size("cross")
    me = lax.axis_index("slab") * cross_count + lax.axis_index("cross")
    edge = COARSE
    slabs = edge // planes
    quarter = columns // 4
    squared = edge * edge
    width = squared // LANES
    lane = lax.broadcasted_iota(jnp.int32, (8, LANES), 1)
    row = lax.broadcasted_iota(jnp.int32, (8, LANES), 0)
    sixth = 1.0 / 6.0

    pitch = width + 1

    def at_plane(plane, v):
        return pl.ds((plane + 1) * pitch + v, 8, stride=pitch)

    for i in (0, slabs + 1):
        ends[i] = jnp.zeros(ends.shape[1:], F32)
    for ref in (one, two):
        for start in (0, (edge + 1) * pitch):
            ref[pl.ds(start, pitch), :] = jnp.zeros((pitch, LANES), F32)
    for part, part_masks in zip(parts, masks):
        for i, mask in enumerate(part_masks):
            owner = lax.bitwise_xor(me, mask)
            slab = owner // cross_count
            cross = lax.rem(owner, cross_count)
            at = pl.ds(pl.multiple_of(cross * columns, LANES), columns)
            source[slab, :, at] = part[i, :, :columns]
            at = pl.ds(pl.multiple_of(cross * quarter, LANES), quarter)
            ends[slab + 1, :, at] = part[i, :, columns:]

    def at_lanes(v):
        return pl.ds(v * LANES, LANES)

    def begin(s, _):
        for v in range(width):
            j, l = v * LANES % columns // quarter, v * LANES % quarter
            here = pl.ds(v * LANES // columns * quarter + l, LANES)
            above = jnp.broadcast_to(ends[s + 2, j : j + 1, here], (8, LANES))
            under = jnp.broadcast_to(ends[s, 4 + j : 5 + j, here], (8, LANES))
            x = source[s, :, at_lanes(v)]
            x = x + jnp.where(row == 7, above, jnp.where(row == 0, under, 0.0))
            source[s, :, at_lanes(v)] = x
            one[at_plane(s * 8, v), :] = x * sixth
        return 0

    lax.fori_loop(0, slabs, begin, 0)

    k = lax.broadcasted_iota(jnp.int32, (2 * LANES, 2 * LANES), 0) % LANES
    l = lax.broadcasted_iota(jnp.int32, (2 * LANES, 2 * LANES), 1)
    crossed = k == lax.rem(l + edge, LANES)
    beside = (jnp.abs(k - l) == 1) & (k // edge == l // edge)
    near = jnp.where(crossed | beside, 1.0, 0.0).astype(jnp.bfloat16)

    def multiply(src, group, products):
        x = jnp.concatenate(
            [
                src[at_plane(s * 8, v), :]
                for s in range(group * GROUP, (group + 1) * GROUP)
                for v in range(width)
            ],
            axis=0,
        )
        high = x.astype(jnp.bfloat16)
        middle = (x - high.astype(F32)).astype(jnp.bfloat16)
        products[...] = jnp.dot(
            jnp.concatenate([high, middle], axis=1), near, preferred_element_type=F32
        )

    def combine(src, group, products, put):
        for i in range(GROUP):
            s = group * GROUP + i
            base = i * width * 8

            def turned(v):
                if 0 <= v < width:
                    return products[base + v * 8 : base + v * 8 + 8, LANES:]
                return jnp.zeros((8, LANES), F32)

            for v in range(width):
                total = source[s, :, at_lanes(v)] + products[base + v * 8 : base + v * 8 + 8, :LANES]
                total = total + jnp.where(lane < edge, turned(v - 1), turned(v + 1))
                total = total + src[at_plane(s * 8 + 1, v), :] + src[at_plane(s * 8 - 1, v), :]
                put(s, v, total * sixth)
            if put is final:
                leave(s).start()

    def sweep(src, put):
        groups = slabs // GROUP
        multiply(src, 0, even_products)
        for g in range(groups):
            now, later = (even_products, odd_products)[:: 1 if g % 2 == 0 else -1]
            if g + 1 < groups:
                multiply(src, g + 1, later)
            combine(src, g, now, put)

    def into(ref):
        def put(s, v, x):
            ref[at_plane(s * 8, v), :] = x

        return put

    def final(s, v, x):
        done[s, :, at_lanes(v)] = x

    def leave(s):
        rows = pl.ds(pl.multiple_of(s * 8, 8), 8)
        return pltpu.make_async_copy(done.at[s], out.at[rows], sems.at[s])

    buffers = (one, two)
    for step in range(1, SWEEPS):
        src = buffers[(step - 1) % 2]
        sweep(src, final if step == SWEEPS - 1 else into(buffers[step % 2]))
    for s in range(slabs):
        leave(s).wait()


def neighbour_pairs(slab_count, cross_count, start):
    pairs = []
    for s in range(start, slab_count - 1, 2):
        for c in range(cross_count):
            i, j = s * cross_count + c, (s + 1) * cross_count + c
            pairs += [(i, j), (j, i)]
    return pairs


def body(gas_state, parcel_record, condensed_shares, surface_steam_factor, fine_cell, block_counts):
    fields, planes, cells = gas_state.shape
    slots = parcel_record.shape[1]
    slab_count = lax.axis_size("slab")
    cross_count = lax.axis_size("cross")
    device_count = slab_count * cross_count
    squared = COARSE * COARSE
    fine_per_coarse = planes * slab_count // COARSE
    columns = cells * cross_count // squared
    columns = cells // columns
    per_plane = cells // LANES
    inner = planes * per_plane
    blocks = slots // BLOCK
    pairs_a = neighbour_pairs(slab_count, cross_count, 0)
    pairs_b = neighbour_pairs(slab_count, cross_count, 1)

    def swap(a, b):
        return lax.ppermute(a, AXES, pairs_a), lax.ppermute(b, AXES, pairs_b)

    plane = jax.ShapeDtypeStruct((per_plane, fields, LANES), F32)
    cell_rows = fine_cell.reshape(blocks, LANES)
    inputs = (
        gas_state, parcel_record, condensed_shares, cell_rows, block_counts, surface_steam_factor,
    )
    *held, edge_a, edge_b = pl.pallas_call(
        load_kernel,
        out_shape=tuple(jax.ShapeDtypeStruct(x.shape, x.dtype) for x in inputs) + (plane, plane),
        in_specs=[HBM] * 6, out_specs=(VMEM,) * 8,
        scratch_shapes=[pltpu.SemaphoreType.DMA((PIECES + 5,))],
        name="load", compiler_params=room(8),
    )(*[pltpu.with_memory_space_constraint(x, pltpu.HBM) for x in inputs])
    gas_state, parcel_record, condensed_shares, cell_rows, block_counts, steam = held
    got_a, got_b = swap(edge_a, edge_b)
    total_tiles = inner + 2 * per_plane + WIDE
    all_tiles = jax.ShapeDtypeStruct((total_tiles, fields, LANES), F32)
    record = jax.ShapeDtypeStruct(parcel_record.shape, F32)
    scalars = jnp.concatenate(
        [cell_rows[:, 0] // LANES, cell_rows[:, LANES - 1] // LANES, block_counts]
    )
    scalars = (scalars, steam)
    partial = pl.pallas_call(
        interior_kernel,
        out_shape=(record, all_tiles, all_tiles),
        in_specs=[SMEM] * 2 + [VMEM] * 4,
        out_specs=(VMEM,) * 3,
        name="interior", compiler_params=room(16),
    )(*scalars, cell_rows, gas_state, parcel_record, condensed_shares)
    updated, acc, send_a, send_b, coarse = pl.pallas_call(
        border_kernel,
        out_shape=(
            record,
            all_tiles,
            plane,
            plane,
            jax.ShapeDtypeStruct((8, columns + columns // 4), F32),
        ),
        in_specs=[SMEM] * 2 + [VMEM] * 8,
        out_specs=(VMEM,) * 5,
        scratch_shapes=[pltpu.VMEM((2 * per_plane, fields, LANES), F32)],
        name="border", compiler_params=room(16),
    )(*scalars, cell_rows, got_a, got_b, parcel_record, condensed_shares, *partial)
    back_a, back_b = swap(send_a, send_b)
    fine_source, parcel_next = pl.pallas_call(
        merge_kernel,
        out_shape=(jax.ShapeDtypeStruct(gas_state.shape, F32), record),
        in_specs=[VMEM] * 4, out_specs=(VMEM, VMEM), name="merge", compiler_params=room(12),
    )(acc, back_a, back_b, updated)

    own_planes = planes
    if fine_per_coarse != 1:
        coarse, own_planes = shared_planes(coarse, columns, planes, fine_per_coarse)
    parts, masks = gather_all(coarse, device_count)
    if fine_per_coarse == 1:
        slabs = COARSE // planes
        products = pltpu.VMEM((GROUP * planes * squared // LANES, 2 * LANES), F32)
        padded = pltpu.VMEM(((COARSE + 2) * (squared // LANES + 1), LANES), F32)
        correction = pl.pallas_call(
            functools.partial(relax_kernel, masks, columns),
            out_shape=jax.ShapeDtypeStruct((COARSE, squared), F32),
            in_specs=[VMEM] * len(parts),
            out_specs=pl.BlockSpec(memory_space=pl.ANY),
            scratch_shapes=[
                pltpu.VMEM((slabs, planes, squared), F32),
                pltpu.VMEM((slabs + 2, 8, squared // 4), F32),
                padded,
                padded,
                pltpu.VMEM((slabs, planes, squared), F32),
                products,
                products,
                pltpu.SemaphoreType.DMA((slabs,)),
            ],
            name="relax", compiler_params=room(16),
        )(*parts)
    else:
        correction = relax_plain(arrange(parts, masks, columns, own_planes, fine_per_coarse, planes))
    return (parcel_next, fine_source, correction)


def gather_all(x, device_count):
    bits = list(range(device_count.bit_length() - 1))[::-1]
    groups = []
    upper = bits[:-1]
    if len(upper) % 2:
        groups.append(upper[:1])
        upper = upper[1:]
    groups += [upper[i : i + 2] for i in range(0, len(upper), 2)]
    held, masks = [x[None]], [[0]]

    def send(part, mask):
        return lax.ppermute(part, AXES, [(i, i ^ mask) for i in range(device_count)])

    for group in groups:
        steps = [1 << group[0]]
        if len(group) == 2:
            steps += [1 << group[1], (1 << group[0]) + (1 << group[1])]
        if len(held) > 1:
            held = [jnp.concatenate(held, axis=0)]
            masks = [[m for part in masks for m in part]]
        held = held + [send(held[0], mask) for mask in steps]
        masks = masks + [[m ^ mask for m in masks[0]] for mask in steps]
    held = held + [send(part, 1) for part in held]
    return tuple(held), tuple(masks + [[m ^ 1 for m in part] for part in masks])


def shared_planes(coarse, columns, planes, fine_per_coarse):
    slab_count = lax.axis_size("slab")
    slab_index = lax.axis_index("slab")
    own = coarse[:, :columns]
    ends = coarse[:, columns:].reshape(2, columns)
    up = [(i, i + 1) for i in range(slab_count - 1)]
    down = [(j, i) for i, j in up]
    own = own.at[planes - 1].add(lax.ppermute(ends[0], "slab", down))
    own = own.at[0].add(lax.ppermute(ends[1], "slab", up))
    if fine_per_coarse <= planes:
        own = own.reshape(planes // fine_per_coarse, fine_per_coarse, columns).sum(axis=1)
        return own.reshape(-1, LANES), planes // fine_per_coarse
    own = own.sum(axis=0)
    group = fine_per_coarse // planes
    for level in range(group.bit_length() - 2, -1, -1):
        half = own.shape[0] // 2
        upper_side = slab_index // 2**level % 2 == 1
        keep = jnp.where(upper_side, own[half:], own[:half])
        send = jnp.where(upper_side, own[:half], own[half:])
        pairs = [(i, i ^ 1 << level) for i in range(slab_count)]
        own = keep + lax.ppermute(send, "slab", pairs)
    return own.reshape(-1, LANES), 1


def arrange(parts, masks, columns, own_planes, fine_per_coarse, planes):
    slab_count = lax.axis_size("slab")
    cross_count = lax.axis_size("cross")
    me = lax.axis_index("slab") * cross_count + lax.axis_index("cross")
    rows = jnp.concatenate(parts, axis=0)
    rows = rows.reshape(rows.shape[0], -1)
    distance = jnp.array([m for part in masks for m in part], jnp.int32)
    position = jnp.argsort(distance)[lax.bitwise_xor(me, jnp.arange(rows.shape[0]))]
    rows = rows[position]
    if fine_per_coarse <= planes:
        rows = rows.reshape(slab_count, cross_count, own_planes, columns)
    else:
        group = fine_per_coarse // planes
        rows = rows.reshape(COARSE, group, cross_count, columns // group)
    return jnp.transpose(rows, (0, 2, 1, 3)).reshape(COARSE, COARSE * COARSE)


def neighbours(grid):
    edge = grid.shape[0]
    x = jnp.pad(grid, ((1, 1), (0, 0)))
    y = jnp.pad(grid, ((0, 0), (edge, edge)))
    z = jnp.pad(grid, ((0, 0), (1, 1)))
    depth = jnp.arange(grid.shape[1], dtype=jnp.int32) % edge
    total = x[2:] + x[:-2] + y[:, 2 * edge :] + y[:, : -2 * edge]
    return total + jnp.where(depth < edge - 1, z[:, 2:], 0.0) + jnp.where(depth > 0, z[:, :-2], 0.0)


def relax_plain(coarse_source):
    correction = jnp.zeros_like(coarse_source)
    for _ in range(SWEEPS):
        correction = (neighbours(correction) + coarse_source) / 6.0
    return correction


def solution(mesh):
    in_specs = (
        P(None, "slab", "cross"),
        P(None, ("slab", "cross")),
        P(None, ("slab", "cross")),
        P(),
        P(("slab", "cross")),
        P(("slab", "cross")),
    )
    out_specs = (P(None, ("slab", "cross")), P(None, "slab", "cross"), P())

    def step(*args):
        return body(*args)

    step = jax.shard_map(step, mesh=mesh, in_specs=in_specs, out_specs=out_specs, check_vma=False)
    return step
```

```python
import functools

import jax
import jax.numpy as jnp
from jax import lax
from jax.experimental import pallas as pl
from jax.experimental.pallas import tpu as pltpu
from jax.sharding import PartitionSpec as P


BLOCK = 128
COARSE = 64
SWEEPS = 4
LANES = 128
WIDE = 8
UNROLL = 4
PIECES = 2
GROUP = 2
AXES = ("slab", "cross")
F32 = jnp.float32
VMEM = pl.BlockSpec(memory_space=pltpu.VMEM)
HBM = pl.BlockSpec(memory_space=pltpu.HBM)


def room(mib):
    return pltpu.CompilerParams(vmem_limit_bytes=mib * 2**20)


drag_rate = 0.5
evap_rate = 0.08
warming_speed = 0.3
latent_boiling_energy = 0.5
vapour_heat = 1.5
volume_inverse = 4.0


def rows_in(tile, species):
    return jnp.concatenate([tile[:, 4 : 4 + species], tile[:, 0:4]], axis=1)


def plane_sides():
    return lax.rem(lax.axis_index("slab"), 2) == 0


def load_kernel(
    gas_in, record_in, shares_in, rows_in_hbm, count_in, steam_in,
    gas, record, shares, rows, count, steam, first_pair, second_pair, steam_s, sems,
):
    fields, planes, cells = gas.shape
    step = fields // PIECES
    moves = [(gas_in.at[pl.ds(i * step, step)], gas.at[pl.ds(i * step, step)]) for i in range(PIECES)]
    moves += [
        (record_in, record), (shares_in, shares),
        (rows_in_hbm, rows), (count_in, count), (steam_in, steam_s),
    ]
    copies = [
        pltpu.make_async_copy(source, target, sems.at[i])
        for i, (source, target) in enumerate(moves)
    ]
    for copy in copies:
        copy.start()
    even = plane_sides()
    for copy in copies[:PIECES]:
        copy.wait()
    for k in range(cells // LANES):
        x = jnp.swapaxes(gas[:, :, k * LANES : (k + 1) * LANES], 0, 1)
        low, high = (rows_in(x[p : p + 1], fields - 4)[0] for p in (0, planes - 1))
        first_pair[k] = jnp.where(even, high, low)
        second_pair[k] = jnp.where(even, low, high)
    for copy in copies[PIECES:]:
        copy.wait()
    species_row = lax.broadcasted_iota(jnp.int32, steam.shape, 0)
    spread = jnp.zeros(steam.shape, F32)
    for j in range(shares.shape[0]):
        spread = jnp.where(species_row == j, steam_s[j], spread)
    steam[...] = spread


def advance_block(g, record, shares, steam, count):
    species = shares.shape[0]
    lane = lax.broadcasted_iota(jnp.int32, (1, LANES), 1)
    row = lax.broadcasted_iota(jnp.int32, (8, LANES), 0)
    rest = species - 8
    zeros = jnp.zeros((8 - rest, LANES), F32)
    g0, g1 = g
    s0 = shares[0:8]
    s1 = jnp.concatenate([shares[8:species], zeros], axis=0)
    r = jnp.concatenate([zeros, record[0:4]], axis=0)
    thermal = record[3:4]
    mass = record[4:5]
    d = g1 - r
    moving = (row >= 4) & (row < 7)
    slip_squared = jnp.sum(jnp.where(moving, d * d, 0.0), axis=0, keepdims=True)
    log_mass = jnp.log(mass)
    drag = (
        drag_rate
        * jnp.exp(log_mass * (-2.0 / 3.0))
        * (1.0 + 0.15 * jnp.exp(0.3435 * jnp.log(slip_squared + 1.0)))
    )
    following = (r + drag * g1) / (1.0 + drag)
    vapour = jnp.exp(2.0 * (thermal - 0.75))
    scale = evap_rate * mass
    rate0 = scale * (s0 * steam[0:8] * vapour - g0)
    rate1 = scale * (s1 * steam[8:16] * vapour - g1)
    evap = jnp.sum(rate0 + jnp.where(row < rest, rate1, 0.0), axis=0, keepdims=True)
    heat = warming_speed * d[7:8] * jnp.exp(log_mass * (1.0 / 3.0))
    next_thermal = thermal + (heat - latent_boiling_energy * evap) / mass
    next_mass = mass - evap
    momentum = mass * (r - following) + evap * following
    energy = vapour_heat * evap - heat
    alive = lane < count
    weight = jnp.where(alive, volume_inverse, 0.0)
    terms0 = rate0 * weight
    terms1 = jnp.where(row < rest, rate1, jnp.where(row < 7, momentum, energy)) * weight
    updated = jnp.concatenate([following[4:7], next_thermal, next_mass], axis=0)
    return (terms0, terms1), jnp.where(alive, updated, record)


def three_parts(x):
    high = x.astype(jnp.bfloat16).astype(F32)
    x = x - high
    middle = x.astype(jnp.bfloat16).astype(F32)
    return high, middle, x - middle


def deposit(parts, tile_of, first, onehot, number, acc):
    stack = []
    for j in range(number):
        here = tile_of == first + j
        for t0, t1 in parts:
            both = jnp.concatenate([jnp.where(here, t0, 0.0), jnp.where(here, t1, 0.0)], axis=0)
            stack.append(both.astype(jnp.bfloat16))
    stack = jnp.concatenate(stack, axis=0)
    sums = lax.dot_general(
        stack, onehot, (((1,), (1,)), ((), ())), preferred_element_type=F32
    )
    rows = 16
    for j in range(number):
        base = j * len(parts) * rows
        total = sums[base : base + rows]
        for i in range(1, len(parts)):
            total = total + sums[base + i * rows : base + (i + 1) * rows]
        acc[first + j] = acc[first + j] + total


def tile_number(cell):
    return lax.shift_right_logical(cell, LANES.bit_length() - 1)


def run_groups(wanted, scalar_s, steam_v, cell_v, record, shares, next_record, acc, gas):
    blocks = cell_v.shape[0]
    steam = steam_v[...]
    spot = lax.broadcasted_iota(jnp.int32, (LANES, LANES), 0)
    zero = jnp.zeros((8, LANES), F32)

    def prepare(b):
        cell = cell_v[pl.ds(b, 1), :]
        offset = lax.bitwise_and(cell, LANES - 1)
        return tile_number(cell), jnp.broadcast_to(offset, (8, LANES))

    def pick(tile, tile_of, offset, number, old):
        here = tile_of == number
        return tuple(
            jnp.where(here, jnp.take_along_axis(tile[h * 8 : h * 8 + 8], offset, axis=1), o)
            for h, o in enumerate(old)
        )

    def advance(b, g):
        at = pl.ds(pl.multiple_of(b * LANES, LANES), LANES)
        terms, new = advance_block(g, record[:, at], shares[:, at], steam, scalar_s[2 * blocks + b])
        next_record[:, at] = new
        return tuple(zip(*(three_parts(t) for t in terms)))

    def hot(offset):
        return jnp.where(spot == offset[0:1], 1.0, 0.0).astype(jnp.bfloat16)

    def span(b):
        return scalar_s[b], scalar_s[blocks + b]

    def group(i, _):
        base = i * UNROLL
        spans = [span(base + u) for u in range(UNROLL)]
        chosen = wanted(spans[0][0], spans[-1][1])
        narrow = functools.reduce(
            jnp.logical_and, [last - first < WIDE for first, last in spans]
        )

        @pl.when(chosen & narrow)
        def _():
            staged = []
            for u in range(UNROLL):
                first = spans[u][0]
                tile_of, offset = prepare(base + u)
                g = (zero, zero)
                for j in range(WIDE):
                    g = pick(gas(first + j), tile_of, offset, first + j, g)
                staged.append((first, tile_of, offset, g))
            staged = [
                (first, tile_of, offset, advance(base + u, g))
                for u, (first, tile_of, offset, g) in enumerate(staged)
            ]
            for first, tile_of, offset, parts in staged:
                deposit(parts, tile_of, first, hot(offset), WIDE, acc)

        @pl.when(chosen & jnp.logical_not(narrow))
        def _():
            def one(u, _):
                b = base + u
                first, last = span(b)
                tile_of, offset = prepare(b)

                def step(t, g):
                    return pick(gas(t), tile_of, offset, t, g)

                g = lax.fori_loop(first, last + 1, step, (zero, zero))
                parts = advance(b, g)
                onehot = hot(offset)

                def put(t, _):
                    deposit(parts, tile_of, t, onehot, 1, acc)
                    return 0

                return lax.fori_loop(first, last + 1, put, 0)

            lax.fori_loop(0, UNROLL, one, 0)

        return 0

    lax.fori_loop(0, blocks // UNROLL, group, 0)


def inside_planes(per_plane, inner):
    return lambda first, last: (first >= per_plane) & (last < per_plane + inner)


def interior_kernel(
    scalar_v, steam_v, cell_v, gas_state, record, shares, next_record, acc, gas, scalar_s, sem
):
    fetch = pltpu.make_async_copy(scalar_v, scalar_s, sem)
    fetch.start()
    fields, planes, cells = gas_state.shape
    per_plane = cells // LANES
    inner = planes * per_plane

    def clear(i, _):
        for u in range(8):
            acc[i * 8 + u] = jnp.zeros(acc.shape[1:], F32)
        return 0

    lax.fori_loop(0, acc.shape[0] // 8, clear, 0)
    for k in range(per_plane):
        x = jnp.swapaxes(gas_state[:, :, k * LANES : (k + 1) * LANES], 0, 1)
        x = rows_in(x, fields - 4)
        for p in range(planes):
            gas[(p + 1) * per_plane + k] = x[p]
    fetch.wait()
    run_groups(
        inside_planes(per_plane, inner),
        scalar_s, steam_v, cell_v, record, shares, next_record, acc, lambda t: gas[t],
    )


def border_kernel(
    scalar_v, steam_v, cell_v, pair_a, pair_b, record, shares,
    record_before, acc_before, gas_before, next_record, acc, send_a, send_b, coarse,
    halo, scalar_s, sem,
):
    fetch = pltpu.make_async_copy(scalar_v, scalar_s, sem)
    fetch.start()
    per_plane = pair_a.shape[0]
    inner = acc.shape[0] - 2 * per_plane - WIDE
    next_record[...] = record_before[...]
    for i in range(0, acc.shape[0], 8):
        acc[i : i + 8] = acc_before[i : i + 8]
    species = shares.shape[0]
    even = plane_sides()
    for k in range(per_plane):
        a, b = pair_a[k], pair_b[k]
        halo[k] = jnp.where(even, b, a)
        halo[per_plane + k] = jnp.where(even, a, b)

    def gas(t):
        low = t < per_plane
        high = t >= per_plane + inner
        place = jnp.where(high, t - inner, jnp.where(low, t, 0))
        return jnp.where(low | high, halo[place], gas_before[t])

    within = inside_planes(per_plane, inner)
    fetch.wait()
    run_groups(
        lambda first, last: jnp.logical_not(within(first, last)),
        scalar_s, steam_v, cell_v, record, shares, next_record, acc, gas,
    )
    for k in range(per_plane):
        low, high = acc[k], acc[per_plane + inner + k]
        send_a[k] = jnp.where(even, high, low)
        send_b[k] = jnp.where(even, low, high)

    planes = inner // per_plane
    lane = lax.broadcasted_iota(jnp.int32, (8, LANES), 1)
    take = lax.rem(lane * 2, LANES)
    row = lax.broadcasted_iota(jnp.int32, (1, 16, 1), 1)

    def mass_of(stack):
        return jnp.sum(jnp.where(row < species, stack, 0.0), axis=1) * (1.0 / volume_inverse)

    def paired(stack):
        mass = mass_of(stack)
        both = mass + pltpu.roll(mass, LANES - 1, axis=1)
        return jnp.take_along_axis(both, take, axis=1)

    def join(left, right):
        return jnp.where(lane[: left.shape[0]] < LANES // 2, left, right)

    own = [
        paired(jnp.stack([acc[(p + 1) * per_plane + k] for p in range(planes)]))
        for k in range(per_plane)
    ]
    for i in range(per_plane // 2):
        coarse[:, i * LANES : (i + 1) * LANES] = join(own[2 * i], own[2 * i + 1])
    columns = per_plane // 2 * LANES
    quarter = per_plane // 8
    for g in range(per_plane // 4):
        sides = (0, per_plane + inner)
        tile = paired(jnp.stack([acc[side + 4 * g + j] for side in sides for j in range(4)]))
        for h in range(2):
            for j in range(2):
                i, at = 2 * g + j, 4 * h + 2 * j
                r, c = 4 * h + i // quarter, i % quarter
                coarse[r : r + 1, columns + c * LANES : columns + (c + 1) * LANES] = join(
                    tile[at : at + 1], tile[at + 1 : at + 2]
                )


def merge_kernel(acc, pair_a, pair_b, record_in, out, record):
    record[...] = record_in[...]
    fields, planes, cells = out.shape
    per_plane = cells // LANES
    even = plane_sides()
    for k in range(per_plane):
        a, b = pair_a[k], pair_b[k]
        from_above = jnp.where(even, a, b)
        from_below = jnp.where(even, b, a)
        rows = [acc[(p + 1) * per_plane + k] for p in range(planes)]
        rows[0] = rows[0] + from_below
        rows[planes - 1] = rows[planes - 1] + from_above
        x = jnp.swapaxes(jnp.stack(rows), 0, 1)
        x = jnp.concatenate([x[fields - 4 :], x[: fields - 4]], axis=0)
        out[:, :, k * LANES : (k + 1) * LANES] = x


def relax_kernel(masks, columns, *refs):
    *parts, out, source, ends, one, two, done, even_products, odd_products, sems = refs
    planes = parts[0].shape[1]
    cross_count = lax.axis_size("cross")
    edge = COARSE
    slabs = edge // planes
    quarter = columns // 4
    squared = edge * edge
    width = squared // LANES
    lane = lax.broadcasted_iota(jnp.int32, (8, LANES), 1)
    row = lax.broadcasted_iota(jnp.int32, (8, LANES), 0)
    sixth = 1.0 / 6.0

    pitch = width + 1

    def at_plane(plane, v):
        return pl.ds((plane + 1) * pitch + v, 8, stride=pitch)

    for i in (0, slabs + 1):
        ends[i] = jnp.zeros(ends.shape[1:], F32)
    for ref in (one, two):
        for start in (0, (edge + 1) * pitch):
            ref[pl.ds(start, pitch), :] = jnp.zeros((pitch, LANES), F32)
    for part, part_masks in zip(parts, masks):
        for i, mask in enumerate(part_masks):
            slab = lax.bitwise_xor(lax.axis_index("slab"), mask // cross_count)
            cross = lax.bitwise_xor(lax.axis_index("cross"), mask % cross_count)
            at = pl.ds(pl.multiple_of(cross * columns, LANES), columns)
            source[slab, :, at] = part[i, :, :columns]
            at = pl.ds(pl.multiple_of(cross * quarter, LANES), quarter)
            ends[slab + 1, :, at] = part[i, :, columns:]

    def at_lanes(v):
        return pl.ds(v * LANES, LANES)

    def begin(s, _):
        for v in range(width):
            j, l = v * LANES % columns // quarter, v * LANES % quarter
            here = pl.ds(v * LANES // columns * quarter + l, LANES)
            above = jnp.broadcast_to(ends[s + 2, j : j + 1, here], (8, LANES))
            under = jnp.broadcast_to(ends[s, 4 + j : 5 + j, here], (8, LANES))
            x = source[s, :, at_lanes(v)]
            x = x + jnp.where(row == 7, above, jnp.where(row == 0, under, 0.0))
            source[s, :, at_lanes(v)] = x
            one[at_plane(s * 8, v), :] = x * sixth
        return 0

    lax.fori_loop(0, slabs, begin, 0)

    k = lax.broadcasted_iota(jnp.int32, (2 * LANES, 2 * LANES), 0) % LANES
    l = lax.broadcasted_iota(jnp.int32, (2 * LANES, 2 * LANES), 1)
    crossed = k == lax.rem(l + edge, LANES)
    beside = (jnp.abs(k - l) == 1) & (k // edge == l // edge)
    near = jnp.where(crossed | beside, 1.0, 0.0).astype(jnp.bfloat16)

    def multiply(src, group, products):
        x = jnp.concatenate(
            [
                src[at_plane(s * 8, v), :]
                for s in range(group * GROUP, (group + 1) * GROUP)
                for v in range(width)
            ],
            axis=0,
        )
        high = x.astype(jnp.bfloat16)
        middle = (x - high.astype(F32)).astype(jnp.bfloat16)
        products[...] = jnp.dot(
            jnp.concatenate([high, middle], axis=1), near, preferred_element_type=F32
        )

    def combine(src, group, products, put):
        for i in range(GROUP):
            s = group * GROUP + i
            base = i * width * 8

            def turned(v):
                if 0 <= v < width:
                    return products[base + v * 8 : base + v * 8 + 8, LANES:]
                return jnp.zeros((8, LANES), F32)

            for v in range(width):
                total = source[s, :, at_lanes(v)] + products[base + v * 8 : base + v * 8 + 8, :LANES]
                total = total + jnp.where(lane < edge, turned(v - 1), turned(v + 1))
                total = total + src[at_plane(s * 8 + 1, v), :] + src[at_plane(s * 8 - 1, v), :]
                put(s, v, total * sixth)
            if put is final:
                leave(s).start()

    def sweep(src, put):
        groups = slabs // GROUP
        multiply(src, 0, even_products)
        for g in range(groups):
            now, later = (even_products, odd_products)[:: 1 if g % 2 == 0 else -1]
            if g + 1 < groups:
                multiply(src, g + 1, later)
            combine(src, g, now, put)

    def into(ref):
        def put(s, v, x):
            ref[at_plane(s * 8, v), :] = x

        return put

    def final(s, v, x):
        done[s, :, at_lanes(v)] = x

    def leave(s):
        rows = pl.ds(pl.multiple_of(s * 8, 8), 8)
        return pltpu.make_async_copy(done.at[s], out.at[rows], sems.at[s])

    buffers = (one, two)
    for step in range(1, SWEEPS):
        src = buffers[(step - 1) % 2]
        sweep(src, final if step == SWEEPS - 1 else into(buffers[step % 2]))
    for s in range(slabs):
        leave(s).wait()


def neighbour_pairs(slab_count, cross_count, start):
    pairs = []
    for s in range(start, slab_count - 1, 2):
        for c in range(cross_count):
            i, j = s * cross_count + c, (s + 1) * cross_count + c
            pairs += [(i, j), (j, i)]
    return pairs


def body(gas_state, parcel_record, condensed_shares, surface_steam_factor, fine_cell, block_counts):
    fields, planes, cells = gas_state.shape
    slots = parcel_record.shape[1]
    slab_count = lax.axis_size("slab")
    cross_count = lax.axis_size("cross")
    device_count = slab_count * cross_count
    squared = COARSE * COARSE
    fine_per_coarse = planes * slab_count // COARSE
    columns = cells * cross_count // squared
    columns = cells // columns
    per_plane = cells // LANES
    inner = planes * per_plane
    blocks = slots // BLOCK
    pairs_a = neighbour_pairs(slab_count, cross_count, 0)
    pairs_b = neighbour_pairs(slab_count, cross_count, 1)

    def swap(a, b):
        return lax.ppermute(a, AXES, pairs_a), lax.ppermute(b, AXES, pairs_b)

    plane = jax.ShapeDtypeStruct((per_plane, fields, LANES), F32)
    cell_rows = fine_cell.reshape(blocks, LANES)
    inputs = (
        gas_state, parcel_record, condensed_shares, cell_rows, block_counts, surface_steam_factor,
    )
    *held, edge_a, edge_b = pl.pallas_call(
        load_kernel,
        out_shape=tuple(jax.ShapeDtypeStruct(x.shape, x.dtype) for x in inputs[:-1])
        + (jax.ShapeDtypeStruct((16, LANES), F32), plane, plane),
        in_specs=[HBM] * 6, out_specs=(VMEM,) * 8,
        scratch_shapes=[pltpu.SMEM(surface_steam_factor.shape, F32), pltpu.SemaphoreType.DMA((PIECES + 5,))],
        name="load", compiler_params=room(8),
    )(*[pltpu.with_memory_space_constraint(x, pltpu.HBM) for x in inputs])
    gas_state, parcel_record, condensed_shares, cell_rows, block_counts, steam = held
    got_a, got_b = swap(edge_a, edge_b)
    total_tiles = inner + 2 * per_plane + WIDE
    all_tiles = jax.ShapeDtypeStruct((total_tiles, fields, LANES), F32)
    record = jax.ShapeDtypeStruct(parcel_record.shape, F32)
    scalars = jnp.concatenate(
        [tile_number(cell_rows[:, 0]), tile_number(cell_rows[:, LANES - 1]), block_counts]
    )
    scalars = (scalars, steam)
    partial = pl.pallas_call(
        interior_kernel,
        out_shape=(record, all_tiles, all_tiles),
        in_specs=[VMEM] * 6,
        out_specs=(VMEM,) * 3,
        scratch_shapes=[pltpu.SMEM(scalars[0].shape, jnp.int32), pltpu.SemaphoreType.DMA],
        name="interior", compiler_params=room(16),
    )(*scalars, cell_rows, gas_state, parcel_record, condensed_shares)
    updated, acc, send_a, send_b, coarse = pl.pallas_call(
        border_kernel,
        out_shape=(
            record,
            all_tiles,
            plane,
            plane,
            jax.ShapeDtypeStruct((8, columns + columns // 4), F32),
        ),
        in_specs=[VMEM] * 10,
        out_specs=(VMEM,) * 5,
        scratch_shapes=[
            pltpu.VMEM((2 * per_plane + WIDE, fields, LANES), F32),
            pltpu.SMEM(scalars[0].shape, jnp.int32),
            pltpu.SemaphoreType.DMA,
        ],
        name="border", compiler_params=room(16),
    )(*scalars, cell_rows, got_a, got_b, parcel_record, condensed_shares, *partial)
    back_a, back_b = swap(send_a, send_b)
    fine_source, parcel_next = pl.pallas_call(
        merge_kernel,
        out_shape=(jax.ShapeDtypeStruct(gas_state.shape, F32), record),
        in_specs=[VMEM] * 4, out_specs=(VMEM, VMEM), name="merge", compiler_params=room(12),
    )(acc, back_a, back_b, updated)

    own_planes = planes
    if fine_per_coarse != 1:
        coarse, own_planes = shared_planes(coarse, columns, planes, fine_per_coarse)
    parts, masks = gather_all(coarse, device_count)
    if fine_per_coarse == 1:
        slabs = COARSE // planes
        products = pltpu.VMEM((GROUP * planes * squared // LANES, 2 * LANES), F32)
        padded = pltpu.VMEM(((COARSE + 2) * (squared // LANES + 1), LANES), F32)
        correction = pl.pallas_call(
            functools.partial(relax_kernel, masks, columns),
            out_shape=jax.ShapeDtypeStruct((COARSE, squared), F32),
            in_specs=[VMEM] * len(parts),
            out_specs=pl.BlockSpec(memory_space=pl.ANY),
            scratch_shapes=[
                pltpu.VMEM((slabs, planes, squared), F32),
                pltpu.VMEM((slabs + 2, 8, squared // 4), F32),
                padded,
                padded,
                pltpu.VMEM((slabs, planes, squared), F32),
                products,
                products,
                pltpu.SemaphoreType.DMA((slabs,)),
            ],
            name="relax", compiler_params=room(16),
        )(*parts)
    else:
        correction = relax_plain(arrange(parts, masks, columns, own_planes, fine_per_coarse, planes))
    return (parcel_next, fine_source, correction)


def gather_all(x, device_count):
    bits = list(range(device_count.bit_length() - 1))[::-1]
    groups = []
    upper = bits[:-1]
    if len(upper) % 2:
        groups.append(upper[:1])
        upper = upper[1:]
    groups += [upper[i : i + 2] for i in range(0, len(upper), 2)]
    held, masks = [x[None]], [[0]]

    def send(part, mask):
        return lax.ppermute(part, AXES, [(i, i ^ mask) for i in range(device_count)])

    for group in groups:
        steps = [1 << group[0]]
        if len(group) == 2:
            steps += [1 << group[1], (1 << group[0]) + (1 << group[1])]
        if len(held) > 1:
            held = [jnp.concatenate(held, axis=0)]
            masks = [[m for part in masks for m in part]]
        held = held + [send(held[0], mask) for mask in steps]
        masks = masks + [[m ^ mask for m in masks[0]] for mask in steps]
    held = held + [send(part, 1) for part in held]
    return tuple(held), tuple(masks + [[m ^ 1 for m in part] for part in masks])


def shared_planes(coarse, columns, planes, fine_per_coarse):
    slab_count = lax.axis_size("slab")
    slab_index = lax.axis_index("slab")
    own = coarse[:, :columns]
    ends = coarse[:, columns:].reshape(2, columns)
    up = [(i, i + 1) for i in range(slab_count - 1)]
    down = [(j, i) for i, j in up]
    own = own.at[planes - 1].add(lax.ppermute(ends[0], "slab", down))
    own = own.at[0].add(lax.ppermute(ends[1], "slab", up))
    if fine_per_coarse <= planes:
        own = own.reshape(planes // fine_per_coarse, fine_per_coarse, columns).sum(axis=1)
        return own.reshape(-1, LANES), planes // fine_per_coarse
    own = own.sum(axis=0)
    group = fine_per_coarse // planes
    for level in range(group.bit_length() - 2, -1, -1):
        half = own.shape[0] // 2
        upper_side = slab_index // 2**level % 2 == 1
        keep = jnp.where(upper_side, own[half:], own[:half])
        send = jnp.where(upper_side, own[:half], own[half:])
        pairs = [(i, i ^ 1 << level) for i in range(slab_count)]
        own = keep + lax.ppermute(send, "slab", pairs)
    return own.reshape(-1, LANES), 1


def arrange(parts, masks, columns, own_planes, fine_per_coarse, planes):
    slab_count = lax.axis_size("slab")
    cross_count = lax.axis_size("cross")
    me = lax.axis_index("slab") * cross_count + lax.axis_index("cross")
    rows = jnp.concatenate(parts, axis=0)
    rows = rows.reshape(rows.shape[0], -1)
    distance = jnp.array([m for part in masks for m in part], jnp.int32)
    position = jnp.argsort(distance)[lax.bitwise_xor(me, jnp.arange(rows.shape[0]))]
    rows = rows[position]
    if fine_per_coarse <= planes:
        rows = rows.reshape(slab_count, cross_count, own_planes, columns)
    else:
        group = fine_per_coarse // planes
        rows = rows.reshape(COARSE, group, cross_count, columns // group)
    return jnp.transpose(rows, (0, 2, 1, 3)).reshape(COARSE, COARSE * COARSE)


def neighbours(grid):
    edge = grid.shape[0]
    x = jnp.pad(grid, ((1, 1), (0, 0)))
    y = jnp.pad(grid, ((0, 0), (edge, edge)))
    z = jnp.pad(grid, ((0, 0), (1, 1)))
    depth = jnp.arange(grid.shape[1], dtype=jnp.int32) % edge
    total = x[2:] + x[:-2] + y[:, 2 * edge :] + y[:, : -2 * edge]
    return total + jnp.where(depth < edge - 1, z[:, 2:], 0.0) + jnp.where(depth > 0, z[:, :-2], 0.0)


def relax_plain(coarse_source):
    correction = jnp.zeros_like(coarse_source)
    for _ in range(SWEEPS):
        correction = (neighbours(correction) + coarse_source) / 6.0
    return correction


def solution(mesh):
    in_specs = (
        P(None, "slab", "cross"),
        P(None, ("slab", "cross")),
        P(None, ("slab", "cross")),
        P(),
        P(("slab", "cross")),
        P(("slab", "cross")),
    )
    out_specs = (P(None, ("slab", "cross")), P(None, "slab", "cross"), P())

    def step(*args):
        return body(*args)

    step = jax.shard_map(step, mesh=mesh, in_specs=in_specs, out_specs=out_specs, check_vma=False)
    return step
```

```python
import functools

import jax
import jax.numpy as jnp
from jax import lax
from jax.experimental import pallas as pl
from jax.experimental.pallas import tpu as pltpu
from jax.sharding import PartitionSpec as P


BLOCK = 128
COARSE = 64
SWEEPS = 4
LANES = 128
WIDE = 8
UNROLL = 4
PIECES = 2
GROUP = 2
AXES = ("slab", "cross")
F32 = jnp.float32
VMEM = pl.BlockSpec(memory_space=pltpu.VMEM)
HBM = pl.BlockSpec(memory_space=pltpu.HBM)


def room(mib):
    return pltpu.CompilerParams(vmem_limit_bytes=mib * 2**20)


drag_rate = 0.5
evap_rate = 0.08
warming_speed = 0.3
latent_boiling_energy = 0.5
vapour_heat = 1.5
volume_inverse = 4.0


def rows_in(tile, species):
    return jnp.concatenate([tile[:, 4 : 4 + species], tile[:, 0:4]], axis=1)


def plane_sides():
    return lax.rem(lax.axis_index("slab"), 2) == 0


def load_kernel(
    gas_in, record_in, shares_in, rows_in_hbm, count_in, steam_in,
    gas, record, shares, rows, count, steam, first_pair, second_pair, steam_s, sems,
):
    fields, planes, cells = gas.shape
    step = fields // PIECES
    moves = [(gas_in.at[pl.ds(i * step, step)], gas.at[pl.ds(i * step, step)]) for i in range(PIECES)]
    moves += [
        (record_in, record), (shares_in, shares),
        (rows_in_hbm, rows), (count_in, count), (steam_in, steam_s),
    ]
    copies = [
        pltpu.make_async_copy(source, target, sems.at[i])
        for i, (source, target) in enumerate(moves)
    ]
    for copy in copies:
        copy.start()
    even = plane_sides()
    for copy in copies[:PIECES]:
        copy.wait()
    for k in range(cells // LANES):
        x = jnp.swapaxes(gas[:, :, k * LANES : (k + 1) * LANES], 0, 1)
        low, high = (rows_in(x[p : p + 1], fields - 4)[0] for p in (0, planes - 1))
        first_pair[k] = jnp.where(even, high, low)
        second_pair[k] = jnp.where(even, low, high)
    for copy in copies[PIECES:]:
        copy.wait()
    species_row = lax.broadcasted_iota(jnp.int32, steam.shape, 0)
    spread = jnp.zeros(steam.shape, F32)
    for j in range(shares.shape[0]):
        spread = jnp.where(species_row == j, steam_s[j], spread)
    steam[...] = spread


def advance_block(g, record, shares, steam, count):
    species = shares.shape[0]
    lane = lax.broadcasted_iota(jnp.int32, (1, LANES), 1)
    row = lax.broadcasted_iota(jnp.int32, (8, LANES), 0)
    rest = species - 8
    zeros = jnp.zeros((8 - rest, LANES), F32)
    g0, g1 = g
    s0 = shares[0:8]
    s1 = jnp.concatenate([shares[8:species], zeros], axis=0)
    r = jnp.concatenate([zeros, record[0:4]], axis=0)
    thermal = record[3:4]
    mass = record[4:5]
    d = g1 - r
    moving = (row >= 4) & (row < 7)
    slip_squared = jnp.sum(jnp.where(moving, d * d, 0.0), axis=0, keepdims=True)
    log_mass = jnp.log(mass)
    drag = (
        drag_rate
        * jnp.exp(log_mass * (-2.0 / 3.0))
        * (1.0 + 0.15 * jnp.exp(0.3435 * jnp.log(slip_squared + 1.0)))
    )
    following = (r + drag * g1) / (1.0 + drag)
    vapour = jnp.exp(2.0 * (thermal - 0.75))
    scale = evap_rate * mass
    rate0 = scale * (s0 * steam[0:8] * vapour - g0)
    rate1 = scale * (s1 * steam[8:16] * vapour - g1)
    evap = jnp.sum(rate0 + jnp.where(row < rest, rate1, 0.0), axis=0, keepdims=True)
    heat = warming_speed * d[7:8] * jnp.exp(log_mass * (1.0 / 3.0))
    next_thermal = thermal + (heat - latent_boiling_energy * evap) / mass
    next_mass = mass - evap
    momentum = mass * (r - following) + evap * following
    energy = vapour_heat * evap - heat
    alive = lane < count
    weight = jnp.where(alive, volume_inverse, 0.0)
    terms0 = rate0 * weight
    terms1 = jnp.where(row < rest, rate1, jnp.where(row < 7, momentum, energy)) * weight
    updated = jnp.concatenate([following[4:7], next_thermal, next_mass], axis=0)
    return (terms0, terms1), jnp.where(alive, updated, record)


def two_parts(x):
    high = x.astype(jnp.bfloat16).astype(F32)
    return high, x - high


def deposit(parts, tile_of, first, onehot, number, acc):
    stack = []
    for j in range(number):
        here = tile_of == first + j
        for t0, t1 in parts:
            both = jnp.concatenate([jnp.where(here, t0, 0.0), jnp.where(here, t1, 0.0)], axis=0)
            stack.append(both.astype(jnp.bfloat16))
    stack = jnp.concatenate(stack, axis=0)
    sums = lax.dot_general(
        stack, onehot, (((1,), (1,)), ((), ())), preferred_element_type=F32
    )
    rows = 16
    for j in range(number):
        base = j * len(parts) * rows
        total = sums[base : base + rows]
        for i in range(1, len(parts)):
            total = total + sums[base + i * rows : base + (i + 1) * rows]
        acc[first + j] = acc[first + j] + total


def tile_number(cell):
    return lax.shift_right_logical(cell, LANES.bit_length() - 1)


def run_groups(wanted, scalar_s, steam_v, cell_v, record, shares, next_record, acc, gas):
    blocks = cell_v.shape[0]
    steam = steam_v[...]
    spot = lax.broadcasted_iota(jnp.int32, (LANES, LANES), 0)
    zero = jnp.zeros((8, LANES), F32)

    def prepare(b):
        cell = cell_v[pl.ds(b, 1), :]
        offset = lax.bitwise_and(cell, LANES - 1)
        return tile_number(cell), jnp.broadcast_to(offset, (8, LANES))

    def pick(tile, tile_of, offset, number, old):
        here = tile_of == number
        return tuple(
            jnp.where(here, jnp.take_along_axis(tile[h * 8 : h * 8 + 8], offset, axis=1), o)
            for h, o in enumerate(old)
        )

    def advance(b, g):
        at = pl.ds(pl.multiple_of(b * LANES, LANES), LANES)
        terms, new = advance_block(g, record[:, at], shares[:, at], steam, scalar_s[2 * blocks + b])
        next_record[:, at] = new
        return tuple(zip(*(two_parts(t) for t in terms)))

    def hot(offset):
        return jnp.where(spot == offset[0:1], 1.0, 0.0).astype(jnp.bfloat16)

    def span(b):
        return scalar_s[b], scalar_s[blocks + b]

    def group(i, _):
        base = i * UNROLL
        spans = [span(base + u) for u in range(UNROLL)]
        chosen = wanted(spans[0][0], spans[-1][1])
        narrow = functools.reduce(
            jnp.logical_and, [last - first < WIDE for first, last in spans]
        )

        @pl.when(chosen & narrow)
        def _():
            staged = []
            for u in range(UNROLL):
                first = spans[u][0]
                tile_of, offset = prepare(base + u)
                g = (zero, zero)
                for j in range(WIDE):
                    g = pick(gas(first + j), tile_of, offset, first + j, g)
                staged.append((first, tile_of, offset, g))
            staged = [
                (first, tile_of, offset, advance(base + u, g))
                for u, (first, tile_of, offset, g) in enumerate(staged)
            ]
            for first, tile_of, offset, parts in staged:
                deposit(parts, tile_of, first, hot(offset), WIDE, acc)

        @pl.when(chosen & jnp.logical_not(narrow))
        def _():
            def one(u, _):
                b = base + u
                first, last = span(b)
                tile_of, offset = prepare(b)

                def step(t, g):
                    return pick(gas(t), tile_of, offset, t, g)

                g = lax.fori_loop(first, last + 1, step, (zero, zero))
                parts = advance(b, g)
                onehot = hot(offset)

                def put(t, _):
                    deposit(parts, tile_of, t, onehot, 1, acc)
                    return 0

                return lax.fori_loop(first, last + 1, put, 0)

            lax.fori_loop(0, UNROLL, one, 0)

        return 0

    lax.fori_loop(0, blocks // UNROLL, group, 0)


def inside_planes(per_plane, inner):
    return lambda first, last: (first >= per_plane) & (last < per_plane + inner)


def interior_kernel(
    scalar_v, steam_v, cell_v, gas_state, record, shares, next_record, acc, gas, scalar_s, sem
):
    fetch = pltpu.make_async_copy(scalar_v, scalar_s, sem)
    fetch.start()
    fields, planes, cells = gas_state.shape
    per_plane = cells // LANES
    inner = planes * per_plane

    def clear(i, _):
        for u in range(8):
            acc[i * 8 + u] = jnp.zeros(acc.shape[1:], F32)
        return 0

    lax.fori_loop(0, acc.shape[0] // 8, clear, 0)
    for k in range(per_plane):
        x = jnp.swapaxes(gas_state[:, :, k * LANES : (k + 1) * LANES], 0, 1)
        x = rows_in(x, fields - 4)
        for p in range(planes):
            gas[(p + 1) * per_plane + k] = x[p]
    fetch.wait()
    run_groups(
        inside_planes(per_plane, inner),
        scalar_s, steam_v, cell_v, record, shares, next_record, acc, lambda t: gas[t],
    )


def border_kernel(
    scalar_v, steam_v, cell_v, pair_a, pair_b, record, shares,
    record_before, acc_before, gas_before, next_record, acc, send_a, send_b, coarse,
    halo, scalar_s, sem,
):
    fetch = pltpu.make_async_copy(scalar_v, scalar_s, sem)
    fetch.start()
    per_plane = pair_a.shape[0]
    inner = acc.shape[0] - 2 * per_plane - WIDE
    next_record[...] = record_before[...]
    for i in range(0, acc.shape[0], 8):
        acc[i : i + 8] = acc_before[i : i + 8]
    species = shares.shape[0]
    even = plane_sides()
    for k in range(per_plane):
        a, b = pair_a[k], pair_b[k]
        halo[k] = jnp.where(even, b, a)
        halo[per_plane + k] = jnp.where(even, a, b)

    def gas(t):
        low = t < per_plane
        high = t >= per_plane + inner
        place = jnp.where(high, t - inner, jnp.where(low, t, 0))
        return jnp.where(low | high, halo[place], gas_before[t])

    within = inside_planes(per_plane, inner)
    fetch.wait()
    run_groups(
        lambda first, last: jnp.logical_not(within(first, last)),
        scalar_s, steam_v, cell_v, record, shares, next_record, acc, gas,
    )
    for k in range(per_plane):
        low, high = acc[k], acc[per_plane + inner + k]
        send_a[k] = jnp.where(even, high, low)
        send_b[k] = jnp.where(even, low, high)

    planes = inner // per_plane
    lane = lax.broadcasted_iota(jnp.int32, (8, LANES), 1)
    take = lax.rem(lane * 2, LANES)
    row = lax.broadcasted_iota(jnp.int32, (1, 16, 1), 1)

    def mass_of(stack):
        return jnp.sum(jnp.where(row < species, stack, 0.0), axis=1) * (1.0 / volume_inverse)

    def paired(stack):
        mass = mass_of(stack)
        both = mass + pltpu.roll(mass, LANES - 1, axis=1)
        return jnp.take_along_axis(both, take, axis=1)

    def join(left, right):
        return jnp.where(lane[: left.shape[0]] < LANES // 2, left, right)

    own = [
        paired(jnp.stack([acc[(p + 1) * per_plane + k] for p in range(planes)]))
        for k in range(per_plane)
    ]
    for i in range(per_plane // 2):
        coarse[:, i * LANES : (i + 1) * LANES] = join(own[2 * i], own[2 * i + 1])
    columns = per_plane // 2 * LANES
    quarter = per_plane // 8
    for g in range(per_plane // 4):
        sides = (0, per_plane + inner)
        tile = paired(jnp.stack([acc[side + 4 * g + j] for side in sides for j in range(4)]))
        for h in range(2):
            for j in range(2):
                i, at = 2 * g + j, 4 * h + 2 * j
                r, c = 4 * h + i // quarter, i % quarter
                coarse[r : r + 1, columns + c * LANES : columns + (c + 1) * LANES] = join(
                    tile[at : at + 1], tile[at + 1 : at + 2]
                )


def merge_kernel(acc, pair_a, pair_b, record_in, out, record):
    record[...] = record_in[...]
    fields, planes, cells = out.shape
    per_plane = cells // LANES
    even = plane_sides()
    for k in range(per_plane):
        a, b = pair_a[k], pair_b[k]
        from_above = jnp.where(even, a, b)
        from_below = jnp.where(even, b, a)
        rows = [acc[(p + 1) * per_plane + k] for p in range(planes)]
        rows[0] = rows[0] + from_below
        rows[planes - 1] = rows[planes - 1] + from_above
        x = jnp.swapaxes(jnp.stack(rows), 0, 1)
        x = jnp.concatenate([x[fields - 4 :], x[: fields - 4]], axis=0)
        out[:, :, k * LANES : (k + 1) * LANES] = x


def relax_kernel(masks, columns, *refs):
    *parts, out, source, ends, one, two, done, even_products, odd_products, sems = refs
    planes = parts[0].shape[1]
    cross_count = lax.axis_size("cross")
    edge = COARSE
    slabs = edge // planes
    quarter = columns // 4
    squared = edge * edge
    width = squared // LANES
    lane = lax.broadcasted_iota(jnp.int32, (8, LANES), 1)
    row = lax.broadcasted_iota(jnp.int32, (8, LANES), 0)
    sixth = 1.0 / 6.0

    pitch = width + 1

    def at_plane(plane, v):
        return pl.ds((plane + 1) * pitch + v, 8, stride=pitch)

    for i in (0, slabs + 1):
        ends[i] = jnp.zeros(ends.shape[1:], F32)
    for ref in (one, two):
        for start in (0, (edge + 1) * pitch):
            ref[pl.ds(start, pitch), :] = jnp.zeros((pitch, LANES), F32)
    for part, part_masks in zip(parts, masks):
        for i, mask in enumerate(part_masks):
            slab = lax.bitwise_xor(lax.axis_index("slab"), mask // cross_count)
            cross = lax.bitwise_xor(lax.axis_index("cross"), mask % cross_count)
            at = pl.ds(pl.multiple_of(cross * columns, LANES), columns)
            source[slab, :, at] = part[i, :, :columns]
            at = pl.ds(pl.multiple_of(cross * quarter, LANES), quarter)
            ends[slab + 1, :, at] = part[i, :, columns:]

    def at_lanes(v):
        return pl.ds(v * LANES, LANES)

    def begin(s, _):
        for v in range(width):
            j, l = v * LANES % columns // quarter, v * LANES % quarter
            here = pl.ds(v * LANES // columns * quarter + l, LANES)
            above = jnp.broadcast_to(ends[s + 2, j : j + 1, here], (8, LANES))
            under = jnp.broadcast_to(ends[s, 4 + j : 5 + j, here], (8, LANES))
            x = source[s, :, at_lanes(v)]
            x = x + jnp.where(row == 7, above, jnp.where(row == 0, under, 0.0))
            source[s, :, at_lanes(v)] = x
            one[at_plane(s * 8, v), :] = x * sixth
        return 0

    lax.fori_loop(0, slabs, begin, 0)

    k = lax.broadcasted_iota(jnp.int32, (2 * LANES, 2 * LANES), 0) % LANES
    l = lax.broadcasted_iota(jnp.int32, (2 * LANES, 2 * LANES), 1)
    crossed = k == lax.rem(l + edge, LANES)
    beside = (jnp.abs(k - l) == 1) & (k // edge == l // edge)
    near = jnp.where(crossed | beside, 1.0, 0.0).astype(jnp.bfloat16)

    def multiply(src, group, products):
        x = jnp.concatenate(
            [
                src[at_plane(s * 8, v), :]
                for s in range(group * GROUP, (group + 1) * GROUP)
                for v in range(width)
            ],
            axis=0,
        )
        high = x.astype(jnp.bfloat16)
        middle = (x - high.astype(F32)).astype(jnp.bfloat16)
        products[...] = jnp.dot(
            jnp.concatenate([high, middle], axis=1), near, preferred_element_type=F32
        )

    def combine(src, group, products, put):
        for i in range(GROUP):
            s = group * GROUP + i
            base = i * width * 8

            def turned(v):
                if 0 <= v < width:
                    return products[base + v * 8 : base + v * 8 + 8, LANES:]
                return jnp.zeros((8, LANES), F32)

            for v in range(width):
                total = source[s, :, at_lanes(v)] + products[base + v * 8 : base + v * 8 + 8, :LANES]
                total = total + jnp.where(lane < edge, turned(v - 1), turned(v + 1))
                total = total + src[at_plane(s * 8 + 1, v), :] + src[at_plane(s * 8 - 1, v), :]
                put(s, v, total * sixth)
            if put is final:
                leave(s).start()

    def sweep(src, put):
        groups = slabs // GROUP
        multiply(src, 0, even_products)
        for g in range(groups):
            now, later = (even_products, odd_products)[:: 1 if g % 2 == 0 else -1]
            if g + 1 < groups:
                multiply(src, g + 1, later)
            combine(src, g, now, put)

    def into(ref):
        def put(s, v, x):
            ref[at_plane(s * 8, v), :] = x

        return put

    def final(s, v, x):
        done[s, :, at_lanes(v)] = x

    def leave(s):
        rows = pl.ds(pl.multiple_of(s * 8, 8), 8)
        return pltpu.make_async_copy(done.at[s], out.at[rows], sems.at[s])

    buffers = (one, two)
    for step in range(1, SWEEPS):
        src = buffers[(step - 1) % 2]
        sweep(src, final if step == SWEEPS - 1 else into(buffers[step % 2]))
    for s in range(slabs):
        leave(s).wait()


def neighbour_pairs(slab_count, cross_count, start):
    pairs = []
    for s in range(start, slab_count - 1, 2):
        for c in range(cross_count):
            i, j = s * cross_count + c, (s + 1) * cross_count + c
            pairs += [(i, j), (j, i)]
    return pairs


def body(gas_state, parcel_record, condensed_shares, surface_steam_factor, fine_cell, block_counts):
    fields, planes, cells = gas_state.shape
    slots = parcel_record.shape[1]
    slab_count = lax.axis_size("slab")
    cross_count = lax.axis_size("cross")
    device_count = slab_count * cross_count
    squared = COARSE * COARSE
    fine_per_coarse = planes * slab_count // COARSE
    columns = cells * cross_count // squared
    columns = cells // columns
    per_plane = cells // LANES
    inner = planes * per_plane
    blocks = slots // BLOCK
    pairs_a = neighbour_pairs(slab_count, cross_count, 0)
    pairs_b = neighbour_pairs(slab_count, cross_count, 1)

    def swap(a, b):
        return lax.ppermute(a, AXES, pairs_a), lax.ppermute(b, AXES, pairs_b)

    plane = jax.ShapeDtypeStruct((per_plane, fields, LANES), F32)
    cell_rows = fine_cell.reshape(blocks, LANES)
    inputs = (
        gas_state, parcel_record, condensed_shares, cell_rows, block_counts, surface_steam_factor,
    )
    *held, edge_a, edge_b = pl.pallas_call(
        load_kernel,
        out_shape=tuple(jax.ShapeDtypeStruct(x.shape, x.dtype) for x in inputs[:-1])
        + (jax.ShapeDtypeStruct((16, LANES), F32), plane, plane),
        in_specs=[HBM] * 6, out_specs=(VMEM,) * 8,
        scratch_shapes=[pltpu.SMEM(surface_steam_factor.shape, F32), pltpu.SemaphoreType.DMA((PIECES + 5,))],
        name="load", compiler_params=room(8),
    )(*[pltpu.with_memory_space_constraint(x, pltpu.HBM) for x in inputs])
    gas_state, parcel_record, condensed_shares, cell_rows, block_counts, steam = held
    got_a, got_b = swap(edge_a, edge_b)
    total_tiles = inner + 2 * per_plane + WIDE
    all_tiles = jax.ShapeDtypeStruct((total_tiles, fields, LANES), F32)
    record = jax.ShapeDtypeStruct(parcel_record.shape, F32)
    scalars = jnp.concatenate(
        [tile_number(cell_rows[:, 0]), tile_number(cell_rows[:, LANES - 1]), block_counts]
    )
    scalars = (scalars, steam)
    partial = pl.pallas_call(
        interior_kernel,
        out_shape=(record, all_tiles, all_tiles),
        in_specs=[VMEM] * 6,
        out_specs=(VMEM,) * 3,
        scratch_shapes=[pltpu.SMEM(scalars[0].shape, jnp.int32), pltpu.SemaphoreType.DMA],
        name="interior", compiler_params=room(16),
    )(*scalars, cell_rows, gas_state, parcel_record, condensed_shares)
    updated, acc, send_a, send_b, coarse = pl.pallas_call(
        border_kernel,
        out_shape=(
            record,
            all_tiles,
            plane,
            plane,
            jax.ShapeDtypeStruct((8, columns + columns // 4), F32),
        ),
        in_specs=[VMEM] * 10,
        out_specs=(VMEM,) * 5,
        scratch_shapes=[
            pltpu.VMEM((2 * per_plane + WIDE, fields, LANES), F32),
            pltpu.SMEM(scalars[0].shape, jnp.int32),
            pltpu.SemaphoreType.DMA,
        ],
        name="border", compiler_params=room(16),
    )(*scalars, cell_rows, got_a, got_b, parcel_record, condensed_shares, *partial)
    back_a, back_b = swap(send_a, send_b)
    fine_source, parcel_next = pl.pallas_call(
        merge_kernel,
        out_shape=(jax.ShapeDtypeStruct(gas_state.shape, F32), record),
        in_specs=[VMEM] * 4, out_specs=(VMEM, VMEM), name="merge", compiler_params=room(12),
    )(acc, back_a, back_b, updated)

    own_planes = planes
    if fine_per_coarse != 1:
        coarse, own_planes = shared_planes(coarse, columns, planes, fine_per_coarse)
    parts, masks = gather_all(coarse, device_count)
    if fine_per_coarse == 1:
        slabs = COARSE // planes
        products = pltpu.VMEM((GROUP * planes * squared // LANES, 2 * LANES), F32)
        padded = pltpu.VMEM(((COARSE + 2) * (squared // LANES + 1), LANES), F32)
        correction = pl.pallas_call(
            functools.partial(relax_kernel, masks, columns),
            out_shape=jax.ShapeDtypeStruct((COARSE, squared), F32),
            in_specs=[VMEM] * len(parts),
            out_specs=pl.BlockSpec(memory_space=pl.ANY),
            scratch_shapes=[
                pltpu.VMEM((slabs, planes, squared), F32),
                pltpu.VMEM((slabs + 2, 8, squared // 4), F32),
                padded,
                padded,
                pltpu.VMEM((slabs, planes, squared), F32),
                products,
                products,
                pltpu.SemaphoreType.DMA((slabs,)),
            ],
            name="relax", compiler_params=room(16),
        )(*parts)
    else:
        correction = relax_plain(arrange(parts, masks, columns, own_planes, fine_per_coarse, planes))
    return (parcel_next, fine_source, correction)


def gather_all(x, device_count):
    bits = list(range(device_count.bit_length() - 1))[::-1]
    groups = []
    upper = bits[:-1]
    if len(upper) % 2:
        groups.append(upper[:1])
        upper = upper[1:]
    groups += [upper[i : i + 2] for i in range(0, len(upper), 2)]
    held, masks = [x[None]], [[0]]

    def send(part, mask):
        return lax.ppermute(part, AXES, [(i, i ^ mask) for i in range(device_count)])

    for group in groups:
        steps = [1 << group[0]]
        if len(group) == 2:
            steps += [1 << group[1], (1 << group[0]) + (1 << group[1])]
        if len(held) > 1:
            held = [jnp.concatenate(held, axis=0)]
            masks = [[m for part in masks for m in part]]
        held = held + [send(held[0], mask) for mask in steps]
        masks = masks + [[m ^ mask for m in masks[0]] for mask in steps]
    held = held + [send(part, 1) for part in held]
    return tuple(held), tuple(masks + [[m ^ 1 for m in part] for part in masks])


def shared_planes(coarse, columns, planes, fine_per_coarse):
    slab_count = lax.axis_size("slab")
    slab_index = lax.axis_index("slab")
    own = coarse[:, :columns]
    ends = coarse[:, columns:].reshape(2, columns)
    up = [(i, i + 1) for i in range(slab_count - 1)]
    down = [(j, i) for i, j in up]
    own = own.at[planes - 1].add(lax.ppermute(ends[0], "slab", down))
    own = own.at[0].add(lax.ppermute(ends[1], "slab", up))
    if fine_per_coarse <= planes:
        own = own.reshape(planes // fine_per_coarse, fine_per_coarse, columns).sum(axis=1)
        return own.reshape(-1, LANES), planes // fine_per_coarse
    own = own.sum(axis=0)
    group = fine_per_coarse // planes
    for level in range(group.bit_length() - 2, -1, -1):
        half = own.shape[0] // 2
        upper_side = slab_index // 2**level % 2 == 1
        keep = jnp.where(upper_side, own[half:], own[:half])
        send = jnp.where(upper_side, own[:half], own[half:])
        pairs = [(i, i ^ 1 << level) for i in range(slab_count)]
        own = keep + lax.ppermute(send, "slab", pairs)
    return own.reshape(-1, LANES), 1


def arrange(parts, masks, columns, own_planes, fine_per_coarse, planes):
    slab_count = lax.axis_size("slab")
    cross_count = lax.axis_size("cross")
    me = lax.axis_index("slab") * cross_count + lax.axis_index("cross")
    rows = jnp.concatenate(parts, axis=0)
    rows = rows.reshape(rows.shape[0], -1)
    distance = jnp.array([m for part in masks for m in part], jnp.int32)
    position = jnp.argsort(distance)[lax.bitwise_xor(me, jnp.arange(rows.shape[0]))]
    rows = rows[position]
    if fine_per_coarse <= planes:
        rows = rows.reshape(slab_count, cross_count, own_planes, columns)
    else:
        group = fine_per_coarse // planes
        rows = rows.reshape(COARSE, group, cross_count, columns // group)
    return jnp.transpose(rows, (0, 2, 1, 3)).reshape(COARSE, COARSE * COARSE)


def neighbours(grid):
    edge = grid.shape[0]
    x = jnp.pad(grid, ((1, 1), (0, 0)))
    y = jnp.pad(grid, ((0, 0), (edge, edge)))
    z = jnp.pad(grid, ((0, 0), (1, 1)))
    depth = jnp.arange(grid.shape[1], dtype=jnp.int32) % edge
    total = x[2:] + x[:-2] + y[:, 2 * edge :] + y[:, : -2 * edge]
    return total + jnp.where(depth < edge - 1, z[:, 2:], 0.0) + jnp.where(depth > 0, z[:, :-2], 0.0)


def relax_plain(coarse_source):
    correction = jnp.zeros_like(coarse_source)
    for _ in range(SWEEPS):
        correction = (neighbours(correction) + coarse_source) / 6.0
    return correction


def solution(mesh):
    in_specs = (
        P(None, "slab", "cross"),
        P(None, ("slab", "cross")),
        P(None, ("slab", "cross")),
        P(),
        P(("slab", "cross")),
        P(("slab", "cross")),
    )
    out_specs = (P(None, ("slab", "cross")), P(None, "slab", "cross"), P())

    def step(*args):
        return body(*args)

    step = jax.shard_map(step, mesh=mesh, in_specs=in_specs, out_specs=out_specs, check_vma=False)
    return step
```
